32 devices in a mesh: gx: 4 (over x, core), gy: 8 (over z, y).
Axes of the slice: x: 2, y: 2, z: 4, core: 2. Of those that a mesh axis runs over, the one named last changes fastest.
Arguments:
- velocity: float32 [3, 1024, 512], P(None, ('gx', 'gy')), may hold values from -6 to 6
- depart: float32 [3, 524288], P(None, ('gx', 'gy')), may hold values from -1 to 1
- owner_rank: int32 [524288, 1], P(('gx', 'gy')), may hold values from 0 to 31; in each aligned block of 16384 rows (0 to 16383, 16384 to 32767, ...) at most 1024 rows name the same one
- owner_element_index: int32 [524288], P(('gx', 'gy')), may hold values from 0 to 31
- neighbours: int32 [6, 1024], P(None, ('gx', 'gy')), may hold values from -1 to 1023, as said below
Outputs:
- advected: float32 [3, 1024, 512], P(None, ('gx', 'gy'))
The draws below stay inside these ranges and needn't reach their ends.
Inputs may be any that keep to these rules, and one draw needn't show every extreme that they name: `owner_rank`: within the rows of one device no owner device is named by more than 1024 rows, and in some device's rows one owner is named exactly 1024 times. `neighbours`: -1 marks a boundary face; any other entry is an element of the same block of 32 consecutive elements as the entry's own element, or of the block just before or just after it.
All inputs are finite; a program needn't handle non-finite values.
Results may differ from the reference program's by a relative error of at most 0.0003.
Values sent between devices are 32-bit elements; how exact they have to be, the bound alone decides.
A program may use at most 64 MiB of HBM per device.

```python
import math
import jax
import jax.numpy as jnp
import numpy as np
from jax import lax

VELOCITY_PARTS = 3
NODES = 512
E_DEV = 32
ELEMS = 1024
POINTS = 524288
CAP = 1024
DEVICES = 32


def draw_neighbours(key, part):
    elem_total = ELEMS
    element = jnp.arange(elem_total, dtype=jnp.int32)
    block_of = element // E_DEV
    lowest = jnp.maximum(block_of - 1, 0) * E_DEV
    highest = jnp.minimum(block_of + 2, elem_total // E_DEV) * E_DEV
    pick_key, edge_key = jax.random.split(key)
    offset = jax.random.randint(pick_key, (6, elem_total), 0, 1 << 30, dtype=jnp.int32) % (highest - lowest)[None, :]
    picked = lowest[None, :] + offset
    boundary = jax.random.randint(edge_key, (6, elem_total), 0, 6, dtype=jnp.int32)
    return jnp.where(boundary == 0, -1, picked).astype(jnp.int32)


def place_ends(drawn, rng, least, high):
    spot = [jax.random.randint(jax.random.fold_in(rng, axis), (), 0, length) for axis, length in enumerate(drawn.shape)]
    widest = drawn.shape.index(max(drawn.shape))
    beside = spot[:widest] + [(spot[widest] + 1) % drawn.shape[widest]] + spot[widest + 1:]
    return drawn.at[tuple(spot)].set(least).at[tuple(beside)].set(high)


def shard_levels(rng, shape, shards, smallest, largest):
    level = 1.0
    for axis_at, parts in shards:
        steps = jax.random.uniform(jax.random.fold_in(jax.random.fold_in(rng, 6), axis_at), (parts,), jnp.float32, smallest / len(shards), largest / len(shards))
        level = level * jnp.repeat(jnp.exp(steps), shape[axis_at] // parts).reshape((-1,) + (1,) * (len(shape) - 1 - axis_at))
    return level


def shared_out(rng, own, number, rows, number_of, top, reach, skew):
    ranking = jax.random.permutation(rng, number_of)
    crowded, ordinary = portions_of(number_of, rows * top, reach, skew, True), portions_of(number_of, rows * top, reach, skew, False)
    places = jnp.arange(number_of)

    def named(lengths, turn):
        used = int((lengths > 0).sum())
        fixed = max(1, used // 4)
        moved = fixed + (places - fixed + turn * (used - fixed)) % max(1, number_of - fixed)
        return jnp.zeros((number_of,), jnp.int32).at[ranking[jnp.where(places < fixed, places, moved)]].set(jnp.asarray(lengths, jnp.int32))

    lengths = jnp.where(number % 4 == 0, named(crowded, number // 4), named(ordinary, number - number // 4 - 1))
    mixed = jax.random.permutation(jax.random.fold_in(own, 3), number_of)
    source_of, receiver = mixed[0:number_of // 2 * 2:2], mixed[1:number_of // 2 * 2:2]
    room = jnp.minimum(lengths[source_of] - 1, reach - lengths[receiver]) // 2
    room = jnp.where((source_of == ranking[0]) | (receiver == ranking[0]) | (lengths[receiver] == 0), 0, jnp.maximum(room, 0))
    moved = jax.random.randint(jax.random.fold_in(own, 4), (number_of // 2,), 0, 1 << 20) % (room + 1)
    lengths = lengths.at[source_of].add(-moved).at[receiver].add(moved)
    members = jnp.searchsorted(jnp.cumsum(lengths), jnp.arange(rows * top), side="right").astype(jnp.int32)
    listing = members.reshape(top, rows).T
    listing = listing[jax.random.permutation(jax.random.fold_in(own, 1), rows)]
    turn = jax.random.randint(jax.random.fold_in(own, 2), (rows, 1), 0, top)
    return jnp.take_along_axis(listing, (jnp.arange(top)[None, :] + turn) % top, axis=1)


def portions_of(amount, total, most, lean, full):
    weights = [(1 << 20) // math.isqrt(standing ** lean) + 1 for standing in range(1, amount + 1)]
    largest = most if full else min(most, max(-(-total // amount), total * weights[0] // sum(weights)))
    least = 1 if total - largest >= amount - 1 else 0
    counts, surplus = [largest] + [least] * (amount - 1), total - largest - least * (amount - 1)
    while surplus > 0:
        candidates = [i for i in range(1, amount) if counts[i] < largest] or [i for i in range(1, amount) if counts[i] < most]
        whole, left = sum([weights[i] for i in candidates]), surplus
        for i in candidates:
            extra = min(most - counts[i], max(1, left * weights[i] // whole), surplus)
            counts[i] = counts[i] + extra
            surplus = surplus - extra
    return np.array(counts)


def gaussian(stream_key, extent, scale, limit, cuts=(), kind=jnp.bfloat16):
    values = jax.random.normal(stream_key, extent, jnp.float32) * scale
    if len(cuts) > 0:
        values = shard_levels(stream_key, extent, cuts, -0.22, 0.18) * values
    return jnp.clip(values, min=-limit, max=limit).astype(kind)


def setup_inputs(seed: int = 0) -> dict:
    splits = jax.random.split(jax.random.key(seed), 6)
    velocity = gaussian(splits[0], (VELOCITY_PARTS, ELEMS, NODES), 1.0, 6.0, ((1, 32),), jnp.float32)
    depart = jnp.clip(jax.random.uniform(splits[1], (VELOCITY_PARTS, POINTS), jnp.float32, -1.0, 1.0) * shard_levels(splits[1], (VELOCITY_PARTS, POINTS), ((1, 32),), -0.4, 0.0), -1.0, 1.0)
    owner_rank_keys = jax.random.split(jax.random.fold_in(splits[2], 1), POINTS // (E_DEV * NODES))
    owner_rank_turns = jax.random.permutation(jax.random.fold_in(splits[2], 3), POINTS // (E_DEV * NODES))
    owner_rank = jax.vmap(lambda own, number: shared_out(jax.random.fold_in(splits[2], 2), own, number, E_DEV * NODES, DEVICES, 1, CAP, 2))(owner_rank_keys, owner_rank_turns).reshape((POINTS, 1))
    owner_element_index = place_ends(jax.random.randint(splits[3], (POINTS,), 0, E_DEV), jax.random.fold_in(splits[3], 1), 0, E_DEV - 1).astype(jnp.int32)
    neighbours = draw_neighbours(jax.random.fold_in(splits[5], 71), 0)
    return {"velocity": velocity, "depart": depart, "owner_rank": owner_rank, "owner_element_index": owner_element_index, "neighbours": neighbours}


GLL_POINTS = np.array([-1.0, -0.8717401485096066, -0.5917001814331423, -0.2092992179024789, 0.2092992179024789, 0.5917001814331423, 0.8717401485096066, 1.0])


def lagrange(coords):
    columns = []
    for node_id in range(8):
        factor = jnp.ones_like(coords)
        for other in range(8):
            if other != node_id:
                factor = factor * ((coords - float(GLL_POINTS[other])) / float(GLL_POINTS[node_id] - GLL_POINTS[other]))
        columns.append(factor)
    return jnp.stack(columns, axis=-1)


def face_slicer(face_id):
    whole_range = slice(None)
    edge_at = 7 * (face_id % 2)
    if face_id < 2:
        return (whole_range, whole_range, edge_at)
    if face_id < 4:
        return (whole_range, whole_range, whole_range, edge_at)
    return (whole_range, whole_range, whole_range, whole_range, edge_at)


def faces_of(nodal_cube):
    shape_lead = (nodal_cube.shape[0], nodal_cube.shape[1], 64)
    return jnp.stack([nodal_cube[face_slicer(face_id)].reshape(shape_lead) for face_id in range(6)], axis=1)


def apply_faces(nodal_cube, own_faces, neighbour_faces, local_index, present):
    result = nodal_cube
    for face_id in range(6):
        across_elements = neighbour_faces[:, face_id ^ 1][:, local_index[face_id]]
        change = jnp.where(present[face_id][None, :, None], 0.5 * (across_elements - own_faces[:, face_id]), 0.0)
        result = result.at[face_slicer(face_id)].add(change.reshape(result.shape[0], result.shape[1], 8, 8))
    return result


def reference(velocity, depart, owner_rank, owner_element_index, neighbours):
    owners = (owner_rank[:, 0] * E_DEV + owner_element_index).astype(jnp.int32)
    block_count = POINTS // 4096
    coord_blocks = depart.reshape(3, block_count, 4096).transpose(1, 0, 2)
    owner_blocks = owners.reshape(block_count, 4096)

    def one_block(block_pair):
        coords, owner_row_table = block_pair
        weights = lagrange(coords)
        gathered = jnp.take(velocity, owner_row_table, axis=1).reshape(3, 4096, 8, 8, 8)
        along = jnp.einsum("cbijk,bk->cbij", gathered, weights[2], precision=lax.Precision.HIGHEST)
        rs_plane = weights[0][:, :, None] * weights[1][:, None, :]
        return jnp.sum(along * rs_plane[None], axis=(2, 3))

    departed = lax.map(one_block, (coord_blocks, owner_blocks)).transpose(1, 0, 2)
    nodal_cube = departed.reshape(3, ELEMS, 8, 8, 8)
    own_faces = faces_of(nodal_cube)
    present = neighbours >= 0
    local_index = jnp.maximum(neighbours, 0).astype(jnp.int32)
    result = apply_faces(nodal_cube, own_faces, own_faces, local_index, present)
    return result.reshape(3, ELEMS, 512)
```

```python
import functools

import jax
import jax.numpy as jnp
import numpy as np
from jax import lax
from jax.experimental import pallas as pl
from jax.experimental.pallas import tpu as pltpu
from jax.sharding import PartitionSpec as P

GLL_POINTS = np.array(
    [
        -1.0,
        -0.8717401485096066,
        -0.5917001814331423,
        -0.2092992179024789,
        0.2092992179024789,
        0.5917001814331423,
        0.8717401485096066,
        1.0,
    ]
)
F32, BF16, I32, I16 = jnp.float32, jnp.bfloat16, jnp.int32, jnp.int16
MESH = pl.DeviceIdType.MESH
LANES = 128
GROUPS = 32
PICK_ROWS = 512
FACE_CHUNKS = 4


def lagrange_constants():
    table = np.zeros((8, 8, LANES))
    for i in range(8):
        table[0, i] = 1.0 / np.prod([GLL_POINTS[i] - GLL_POINTS[m] for m in range(8) if m != i])
        for r in range(1, 8):
            table[r, i] = GLL_POINTS[(i + r) % 8]
    return table.astype(np.float32)


def face_selector():
    cube = np.arange(512).reshape(8, 8, 8)
    faces = [cube[0], cube[7], cube[:, 0], cube[:, 7], cube[:, :, 0], cube[:, :, 7]]
    nodes = np.concatenate([face.reshape(-1) for face in faces])
    return (np.arange(512)[:, None] == nodes[None, :]).astype(np.float32)


def round_up(x, to):
    return -(-x // to) * to


def split2(x):
    hi = x.astype(BF16).astype(F32)
    return hi, x - hi


def dot(a, b):
    return lax.dot_general(a, b, (((1,), (0,)), ((), ())), preferred_element_type=F32)


def dot_nt(a, b):
    return lax.dot_general(a, b, (((1,), (1,)), ((), ())), preferred_element_type=F32)


def rows16(row):
    return jnp.broadcast_to(row, (16, row.shape[1])).astype(I16)


def stack(tile, count):
    return jnp.concatenate([tile] * count, axis=0)


def bounded(index, most):
    return jnp.minimum(jnp.maximum(index, 0), most)


def split_position(pos, size):
    group = jnp.floor((pos + 0.5) * (1.0 / size))
    return group, pos - group * size


def positions(peers, tiles_each, code_base, owner_ref, tri_ref, low_ref, pos_ref, meta_ref):
    rows = owner_ref.shape[0]
    wide = meta_ref.shape[1] - LANES
    batch = 8
    owner = owner_ref[...]
    lane = lax.broadcasted_iota(I32, (1, LANES), 1)
    tile_at = lax.broadcasted_iota(I32, (1, wide), 1).astype(F32)

    def step(it, state):
        pos, first, starts, code = state
        hots = [owner == it * batch + q for q in range(batch)]
        ones = jnp.concatenate([jnp.where(hot, 1.0, 0.0) for hot in hots], axis=0).astype(BF16)
        counted = dot(ones, tri_ref[...])
        counts = [counted[rows * q : rows * (q + 1), LANES:] for q in range(batch)]
        before = dot(low_ref[...], jnp.concatenate(counts, axis=1).astype(BF16))
        for q in range(batch):
            earlier = before[:, LANES * q : LANES * (q + 1)]
            slot = counted[rows * q : rows * (q + 1), :LANES] + earlier
            pos = jnp.where(hots[q], slot + (first * LANES - 1.0), pos)
            number = earlier[rows - 1 :] + counts[q][rows - 1 :]
            starts = jnp.where(lane == it * batch + q, first, starts)
            begin = jnp.concatenate([first] * (wide // LANES), axis=1)
            here = code_base(it * batch + q).astype(F32) + jnp.minimum(tile_at - begin, tiles_each - 1.0)
            code = jnp.where(tile_at >= begin, here, code)
            first = first + jnp.floor((number + (LANES - 1.0)) * (1.0 / LANES))
        return pos, first, starts, code

    zero = jnp.zeros((1, LANES), F32)
    state = (jnp.zeros(owner.shape, F32), zero, zero, jnp.zeros((1, wide), F32))
    for it in range(peers // batch):
        state = step(it, state)
    pos, _, starts, code = state
    pos_ref[...] = pos
    meta_ref[...] = jnp.concatenate([starts, code], axis=1).astype(I32)


def place(span, begin, end, pos_ref, coords_ref, elem_ref, row_ref, group_ref, acc):
    size = acc.shape[0]
    wide = group_ref.shape[0]

    @pl.loop(begin, end)
    def _(it):
        hots, spreads = [], []
        for r in range(span):
            row = it * span + r
            group, at = split_position(pos_ref[pl.ds(row, 1), :], size)
            at = stack(rows16(at.astype(I32)), size // 16)
            hots.append(jnp.where(row_ref[0:size, :] == at, jnp.array(1, BF16), jnp.array(0, BF16)))
            lanes = pl.ds(pl.multiple_of(row * LANES, LANES), LANES)
            hi, lo = split2(coords_ref[:, lanes])
            elem = elem_ref[pl.ds(row, 1), :].astype(F32)
            values = jnp.concatenate([hi, elem, lo, jnp.zeros((1, LANES), F32)], axis=0)
            values = stack(stack(values, 2).astype(BF16), wide // 16)
            group = stack(rows16(group.astype(I32)), wide // 16)
            spreads.append(jnp.where(group_ref[...] == group, values, jnp.array(0, BF16)))
        acc[...] += dot_nt(jnp.concatenate(hots, axis=1), jnp.concatenate(spreads, axis=1))


def interpolate(elems, load, store, tiles, chunk, stacked, lag_ref, elem_rows):
    per = chunk // LANES
    for at in range(0, tiles, per):
        x = jnp.concatenate([load(at + t) for t in range(per)], axis=1)
        weights = []
        for d in range(3):
            coord = jnp.broadcast_to(x[d : d + 1], (8, chunk))
            const = [jnp.concatenate([lag_ref[r]] * per, axis=1) for r in range(8)]
            w = const[0] * (coord - const[1])
            for r in range(2, 8):
                w = w * (coord - const[r])
            weights.append(w)
        elem = stack(rows16(x[3:4].astype(I32)), elems // 16)
        pick = jnp.concatenate([elem_rows] * per, axis=1) == elem
        parts = []
        for part in split2(weights[0]):
            pieces = []
            for parity in range(2):
                for m in range(4):
                    i = 2 * m + parity
                    row = stack(jnp.broadcast_to(part[i : i + 1], (16, chunk)).astype(BF16), elems // 16)
                    pieces.append(jnp.where(pick, row, jnp.array(0, BF16)))
            parts.append(jnp.concatenate(pieces, axis=0))
        a_hi, a_lo = parts
        summed = dot(stacked[...], jnp.concatenate([a_hi, a_lo, a_hi], axis=0))
        results = []
        for c in range(3):
            total = None
            for j in range(8):
                term = summed[64 * c + 8 * j : 64 * c + 8 * j + 8] * weights[1][j : j + 1]
                total = term if total is None else total + term
            results.append(jnp.sum(total * weights[2], axis=0, keepdims=True))
        result = jnp.concatenate(results, axis=0)
        for t in range(per):
            store(at + t, result[:, LANES * t : LANES * (t + 1)])


def advect_kernel(
    outer, inner, tiles_each, sorted_tiles, chunk,
    vel_ref, coords_ref, owner_ref, elem_ref, nb_ref, tri_ref, low_ref, lag_ref, sel_ref, sel_t_ref,
    out_ref,
    pos_ref, meta_ref, meta_smem, row_ref, group_ref, acc, sorted_ref, send_ref, table_ref, mirror_ref,
    stacked, arrived, replies, landed, answers, halves, vals, faces, below, above,
    meta_sem, table_out, table_in, go_out, go_in, back_out, back_in, face_out, face_in,
):
    peers = outer * inner
    hin = inner // 2
    half = peers // 2
    elems = vel_ref.shape[1]
    points = coords_ref.shape[1]
    size = acc.shape[0]
    my_x, my_y = lax.axis_index("gx"), lax.axis_index("gy")
    side, low_y = my_y // hin, lax.rem(my_y, hin)
    me = my_x * inner + my_y
    mine = my_x * hin + low_y
    barrier = pltpu.get_barrier_semaphore()

    def place_of(device):
        return (device // inner, lax.rem(device, inner))

    @pl.loop(1, peers)
    def _(s):
        pl.semaphore_signal(barrier, inc=1, device_id=place_of(lax.rem(me + s, peers)), device_id_type=MESH)

    def code_base(p):
        x, y = p // inner, p % inner
        w = lax.rem(y // hin + side, 2)
        return (w * half + x * hin + y % hin) * tiles_each

    positions(peers, tiles_each, code_base, owner_ref, tri_ref, low_ref, pos_ref, meta_ref)
    meta_copy = pltpu.make_async_copy(meta_ref, meta_smem, meta_sem)
    meta_copy.start()

    row_ref[...] = lax.broadcasted_iota(I32, row_ref.shape, 0).astype(I16)
    group_ref[...] = (lax.broadcasted_iota(I32, group_ref.shape, 0) // 8).astype(I16)
    acc[...] = jnp.zeros_like(acc)
    for c in range(3):
        cube = vel_ref[c]
        tall = jnp.concatenate([cube[:, LANES * m : LANES * (m + 1)] for m in range(4)], axis=0).T
        table_ref[64 * c : 64 * (c + 1)] = jnp.concatenate([tall[0:64], tall[64:128]], axis=1)

    span = 8
    steps = points // LANES // span
    place(span, 0, steps // 2, pos_ref, coords_ref, elem_ref, row_ref, group_ref, acc)
    pl.semaphore_wait(barrier, peers - 1)
    table_copy = pltpu.make_async_remote_copy(
        src_ref=table_ref, dst_ref=mirror_ref, send_sem=table_out, recv_sem=table_in,
        device_id=(my_x, lax.rem(my_y + hin, inner)), device_id_type=MESH,
    )
    table_copy.start()
    place(span, steps // 2, steps, pos_ref, coords_ref, elem_ref, row_ref, group_ref, acc)

    per_group = size // LANES
    for j in range(per_group):
        turned = acc[LANES * j : LANES * (j + 1), :].T
        for g in range(GROUPS):
            sorted_ref[g * per_group + j] = turned[8 * g : 8 * g + 8]
    for t in range(GROUPS * per_group, sorted_tiles):
        sorted_ref[t] = jnp.zeros((8, LANES), F32)

    def after(s):
        x, y = lax.rem(my_x + lax.rem(s, outer), outer), lax.rem(low_y + s // outer, hin)
        return x, y

    def before(s):
        x = lax.rem(my_x + outer - lax.rem(s, outer), outer)
        y = lax.rem(low_y + hin - s // outer, hin)
        return x, y

    def block(w, device):
        return pl.ds((w * half + device) * tiles_each, tiles_each)

    def outgoing(w, s, place_at):
        x, y = place_at(s)
        device = x * hin + y
        return device, pltpu.make_async_remote_copy(
            src_ref=send_ref.at[block(w, device)], dst_ref=arrived.at[block(w, mine)],
            send_sem=go_out.at[w, device], recv_sem=go_in.at[w, mine],
            device_id=(x, y + side * hin), device_id_type=MESH,
        )

    def incoming(w, s):
        x, y = before(s)
        device = x * hin + y
        return device, pltpu.make_async_remote_copy(
            src_ref=send_ref.at[block(w, device)], dst_ref=arrived.at[block(w, device)],
            send_sem=go_out.at[w, device], recv_sem=go_in.at[w, device],
            device_id=(x, y + side * hin), device_id_type=MESH,
        )

    def reply(w, s):
        x, y = before(s)
        device = x * hin + y
        return pltpu.make_async_remote_copy(
            src_ref=replies.at[block(w, device)], dst_ref=landed.at[block(w, mine)],
            send_sem=back_out.at[w, device], recv_sem=back_in.at[w, mine],
            device_id=(x, y + side * hin), device_id_type=MESH,
        )

    def answer(w, s):
        x, y = after(s)
        device = x * hin + y
        return pltpu.make_async_remote_copy(
            src_ref=replies.at[block(w, device)], dst_ref=landed.at[block(w, device)],
            send_sem=back_out.at[w, device], recv_sem=back_in.at[w, device],
            device_id=(x, y + side * hin), device_id_type=MESH,
        )

    meta_copy.wait()

    def pack(w, s):
        x, y = after(s)
        owner = x * inner + y + lax.rem(side + w, 2) * hin
        first = bounded(meta_smem[0, owner], sorted_tiles - tiles_each)
        base = (w * half + x * hin + y) * tiles_each
        for k in range(tiles_each):
            send_ref[base + k] = sorted_ref[first + k, 0:4, :] + sorted_ref[first + k, 4:8, :]

    for w in range(2):
        @pl.loop(1, half)
        def _(s):
            pack(w, s)
            outgoing(w, s, after)[1].start()

        pack(w, 0)

    elem_rows = row_ref[0:elems, :]
    for w in range(2):
        if w == 1:
            table_copy.wait_recv()
        hi, lo = split2(table_ref[...] if w == 0 else mirror_ref[...])
        stacked[...] = jnp.concatenate([hi, hi, lo], axis=1).astype(BF16)
        own = (w * half + mine) * tiles_each

        def own_store(t, value):
            landed[own + t, 0:3, :] = value

        interpolate(elems, lambda t: send_ref[own + t], own_store, tiles_each, chunk, stacked, lag_ref, elem_rows)

        @pl.loop(1, half)
        def _(s):
            device, copy = incoming(w, s)
            copy.wait_recv()
            base = (w * half + device) * tiles_each

            def store(t, value):
                replies[base + t, 0:3, :] = value

            interpolate(elems, lambda t: arrived[base + t], store, tiles_each, chunk, stacked, lag_ref, elem_rows)
            reply(w, s).start()

    table_copy.wait_send()
    for w in range(2):
        @pl.loop(1, half)
        def _(s):
            answer(w, s).wait_recv()

    groups = answers.shape[0]
    per_row = PICK_ROWS // LANES
    for g in range(groups):
        for j in range(per_row):
            answers[g, :, LANES * j : LANES * (j + 1)] = landed[
                bounded(meta_smem[0, LANES + g * per_row + j], landed.shape[0] - 1)
            ]
    for c in range(3):
        hi, lo = split2(answers[:, c, :])
        halves[groups * c : groups * (c + 1)] = hi.astype(BF16)
        halves[groups * (c + 3) : groups * (c + 4)] = lo.astype(BF16)

    up, down = lax.rem(me + 1, peers), lax.rem(me + peers - 1, peers)
    face_elems = elems // FACE_CHUNKS
    group_iota = lax.broadcasted_iota(I32, (groups, 512), 0).astype(F32)
    copies = []
    for q in range(FACE_CHUNKS):
        @pl.loop(0, face_elems)
        def _(k):
            e = q * face_elems + k
            pos = jnp.concatenate([pos_ref[pl.ds(4 * e + r, 1), :] for r in range(4)], axis=1)
            group, at = split_position(pos, PICK_ROWS)
            at = stack(rows16(at.astype(I32)), PICK_ROWS // 16)
            rows = jnp.concatenate([row_ref[0:PICK_ROWS, :]] * 4, axis=1)
            picked = dot(halves[...], jnp.where(rows == at, jnp.array(1, BF16), jnp.array(0, BF16)))
            match = group_iota == group
            for c in range(3):
                both = picked[groups * c : groups * (c + 1)] + picked[groups * (c + 3) : groups * (c + 4)]
                vals[c, pl.ds(e, 1), :] = jnp.sum(jnp.where(match, both, 0.0), axis=0, keepdims=True)

        some = slice(q * face_elems, (q + 1) * face_elems)
        hi, lo = split2(jnp.concatenate([vals[c, some, :] for c in range(3)], axis=0))
        both = dot(jnp.concatenate([hi, lo], axis=0).astype(BF16), sel_ref[...])
        both = both[0 : 3 * face_elems] + both[3 * face_elems :]
        for c in range(3):
            faces[q, c] = both[face_elems * c : face_elems * (c + 1)]
        for k, (device, land) in enumerate(((up, below), (down, above))):
            copy = pltpu.make_async_remote_copy(
                src_ref=faces.at[q], dst_ref=land.at[q],
                send_sem=face_out.at[q, k], recv_sem=face_in.at[q, k],
                device_id=place_of(device), device_id_type=MESH,
            )
            copy.start()
            copies.append(copy)

    index = (nb_ref[...] - jnp.where(nb_ref[...] >= 0, (me - 1) * elems, 0)).astype(F32)
    index = jnp.concatenate([index, jnp.zeros((2, elems), F32)], axis=0)
    index = jnp.concatenate([index] * (LANES // elems), axis=1).T[0:elems]
    columns = lax.broadcasted_iota(I32, (elems, 3 * elems), 1).astype(F32)
    column = [jnp.broadcast_to(index[:, f : f + 1], (elems, 3 * elems)) for f in range(6)]
    picker = jnp.concatenate([jnp.where(columns == column[f], 1.0, 0.0) for f in range(6)], axis=0).astype(BF16)
    present = [jnp.where(index[:, f : f + 1] >= 0, 0.5, 0.0) for f in range(6)]

    for w in range(2):
        @pl.loop(1, half)
        def _(s):
            outgoing(w, s, after)[1].wait_send()
            reply(w, s).wait_send()

    for copy in copies:
        copy.wait()

    def whole(ref, c):
        return jnp.concatenate([ref[q, c] for q in range(FACE_CHUNKS)], axis=0)

    changes = []
    for c in range(3):
        own = whole(faces, c)
        extended = jnp.concatenate([whole(below, c), own, whole(above, c)], axis=0)
        hi, lo = split2(extended)
        across = dot(picker, hi.astype(BF16)) + dot(picker, lo.astype(BF16))
        pieces = []
        for f in range(6):
            g = f ^ 1
            rows = slice(f * elems, (f + 1) * elems)
            other = across[rows, 64 * g : 64 * g + 64]
            pieces.append(0.5 * other - present[f] * own[:, 64 * f : 64 * f + 64])
        changes.append(jnp.concatenate(pieces, axis=1))
    hi, lo = split2(jnp.concatenate(changes, axis=0))
    spread = dot(jnp.concatenate([hi, lo], axis=0).astype(BF16), sel_t_ref[...])
    for c in range(3):
        rows = slice(c * elems, (c + 1) * elems)
        out_ref[c] = vals[c] + (spread[rows] + spread[(c + 3) * elems : (c + 4) * elems])


def advect(velocity, coords, owner, elem, neighbours, outer, inner):
    peers = outer * inner
    half = peers // 2
    elems = velocity.shape[1]
    points = coords.shape[1]
    capacity = 2 * points // peers
    tiles_each = capacity // LANES
    used = round_up(points // LANES + peers, GROUPS)
    size = used // GROUPS * LANES
    sorted_tiles = used + tiles_each
    groups = round_up(used * LANES, PICK_ROWS * 8) // PICK_ROWS
    code_lanes = round_up(groups * PICK_ROWS // LANES, LANES)
    tri = np.concatenate([np.triu(np.ones((LANES, LANES))), np.ones((LANES, LANES))], axis=1)
    low = np.tril(np.ones((points // LANES, points // LANES)), -1)
    sel = face_selector()
    face_block = (FACE_CHUNKS, 3, elems // FACE_CHUNKS, 384)
    vmem = pl.BlockSpec(memory_space=pltpu.VMEM)
    return pl.pallas_call(
        functools.partial(advect_kernel, outer, inner, tiles_each, sorted_tiles, min(capacity, 256)),
        in_specs=[vmem] * 10,
        out_specs=vmem,
        out_shape=jax.ShapeDtypeStruct((3, elems, 512), F32),
        scratch_shapes=[
            pltpu.VMEM((points // LANES, LANES), F32),
            pltpu.VMEM((1, LANES + code_lanes), I32),
            pltpu.SMEM((1, LANES + code_lanes), I32),
            pltpu.VMEM((max(size, PICK_ROWS), LANES), I16),
            pltpu.VMEM((GROUPS * 8, LANES), I16),
            pltpu.VMEM((size, GROUPS * 8), F32),
            pltpu.VMEM((sorted_tiles, 8, LANES), F32),
            pltpu.VMEM((peers * tiles_each, 4, LANES), F32),
            pltpu.VMEM((192, elems * 8), F32),
            pltpu.VMEM((192, elems * 8), F32),
            pltpu.VMEM((192, 3 * elems * 8), BF16),
            pltpu.VMEM((peers * tiles_each, 4, LANES), F32),
            pltpu.VMEM((peers * tiles_each, 4, LANES), F32),
            pltpu.VMEM((peers * tiles_each, 4, LANES), F32),
            pltpu.VMEM((groups, 4, PICK_ROWS), F32),
            pltpu.VMEM((6 * groups, PICK_ROWS), BF16),
            pltpu.VMEM((3, elems, 512), F32),
            pltpu.VMEM(face_block, F32),
            pltpu.VMEM(face_block, F32),
            pltpu.VMEM(face_block, F32),
            pltpu.SemaphoreType.DMA,
            pltpu.SemaphoreType.DMA,
            pltpu.SemaphoreType.DMA,
        ]
        + [pltpu.SemaphoreType.DMA((2, half))] * 4
        + [pltpu.SemaphoreType.DMA((FACE_CHUNKS, 2))] * 2,
        compiler_params=pltpu.CompilerParams(collective_id=0, has_side_effects=True),
        name="advect",
    )(
        velocity, coords, owner, elem, neighbours, jnp.asarray(tri, BF16), jnp.asarray(low, BF16),
        jnp.asarray(lagrange_constants()), jnp.asarray(sel, BF16), jnp.asarray(sel.T, BF16),
    )


def local(velocity, depart, owner_rank, owner_element_index, neighbours):
    outer, inner = lax.axis_size("gx"), lax.axis_size("gy")
    rows = depart.shape[1] // LANES
    owner = owner_rank.reshape(rows, LANES)
    elem = owner_element_index.reshape(rows, LANES)
    return advect(velocity, depart, owner, elem, neighbours, outer, inner)


def solution(mesh):
    placed = (
        P(None, ("gx", "gy"), None),
        P(None, ("gx", "gy")),
        P(("gx", "gy"), None),
        P(("gx", "gy")),
        P(None, ("gx", "gy")),
    )
    return jax.shard_map(
        local, mesh=mesh, in_specs=placed, out_specs=P(None, ("gx", "gy"), None), check_vma=False
    )
```

```python
import functools

import jax
import jax.numpy as jnp
import numpy as np
from jax import lax
from jax.experimental import pallas as pl
from jax.experimental.pallas import tpu as pltpu
from jax.sharding import PartitionSpec as P

GLL_POINTS = np.array(
    [
        -1.0,
        -0.8717401485096066,
        -0.5917001814331423,
        -0.2092992179024789,
        0.2092992179024789,
        0.5917001814331423,
        0.8717401485096066,
        1.0,
    ]
)
F32, BF16, I32, I16 = jnp.float32, jnp.bfloat16, jnp.int32, jnp.int16
MESH = pl.DeviceIdType.MESH
LANES = 128
GROUPS = 32
PICK_ROWS = 512
FACE_CHUNKS = 4


def lagrange_constants():
    table = np.zeros((8, 8, LANES))
    for i in range(8):
        table[0, i] = 1.0 / np.prod([GLL_POINTS[i] - GLL_POINTS[m] for m in range(8) if m != i])
        for r in range(1, 8):
            table[r, i] = GLL_POINTS[(i + r) % 8]
    return table.astype(np.float32)


def face_selector():
    cube = np.arange(512).reshape(8, 8, 8)
    faces = [cube[0], cube[7], cube[:, 0], cube[:, 7], cube[:, :, 0], cube[:, :, 7]]
    nodes = np.concatenate([face.reshape(-1) for face in faces])
    return (np.arange(512)[:, None] == nodes[None, :]).astype(np.float32)


def node_split():
    sel = face_selector()
    first = sel * (np.cumsum(sel, axis=1) == 1)
    inside = np.flatnonzero(sel.sum(axis=1) == 0)
    rest = np.zeros((512, round_up(len(inside), LANES)), np.float32)
    rest[inside, np.arange(len(inside))] = 1
    order = np.concatenate([sel, rest], axis=1)
    back = np.concatenate([first, rest], axis=1).T
    return order, back, sel.T


def round_up(x, to):
    return -(-x // to) * to


def split2(x):
    hi = x.astype(BF16).astype(F32)
    return hi, x - hi


def dot(a, b):
    return lax.dot_general(a, b, (((1,), (0,)), ((), ())), preferred_element_type=F32)


def dot_nt(a, b):
    return lax.dot_general(a, b, (((1,), (1,)), ((), ())), preferred_element_type=F32)


def rows16(row):
    return jnp.broadcast_to(row, (16, row.shape[1])).astype(I16)


def stack(tile, count):
    return jnp.concatenate([tile] * count, axis=0)


def bounded(index, most):
    return jnp.minimum(jnp.maximum(index, 0), most)


def split_position(pos, size):
    group = jnp.floor((pos + 0.5) * (1.0 / size))
    return group, pos - group * size


def positions(peers, tiles_each, code_base, owner_ref, tri_ref, low_ref, pos_ref, meta_ref):
    rows = owner_ref.shape[0]
    wide = meta_ref.shape[1] - LANES
    batch = min(peers, 32)
    owner = owner_ref[...]
    lane = lax.broadcasted_iota(I32, (1, LANES), 1)
    tile_at = lax.broadcasted_iota(I32, (1, wide), 1).astype(F32)

    def step(it, state):
        pos, first, starts, code = state
        hots = [owner == it * batch + q for q in range(batch)]
        ones = jnp.concatenate([jnp.where(hot, 1.0, 0.0) for hot in hots], axis=0).astype(BF16)
        counted = dot(ones, tri_ref[...])
        counts = [counted[rows * q : rows * (q + 1), LANES:] for q in range(batch)]
        before = dot(low_ref[...], jnp.concatenate(counts, axis=1).astype(BF16))
        for q in range(batch):
            earlier = before[:, LANES * q : LANES * (q + 1)]
            slot = counted[rows * q : rows * (q + 1), :LANES] + earlier
            pos = jnp.where(hots[q], slot + (first * LANES - 1.0), pos)
            number = earlier[rows - 1 :] + counts[q][rows - 1 :]
            starts = jnp.where(lane == it * batch + q, first, starts)
            begin = jnp.concatenate([first] * (wide // LANES), axis=1)
            here = code_base(it * batch + q).astype(F32) + jnp.minimum(tile_at - begin, tiles_each - 1.0)
            code = jnp.where(tile_at >= begin, here, code)
            first = first + jnp.floor((number + (LANES - 1.0)) * (1.0 / LANES))
        return pos, first, starts, code

    zero = jnp.zeros((1, LANES), F32)
    state = (jnp.zeros(owner.shape, F32), zero, zero, jnp.zeros((1, wide), F32))
    for it in range(peers // batch):
        state = step(it, state)
    pos, _, starts, code = state
    pos_ref[...] = pos
    meta_ref[...] = jnp.concatenate([starts, code], axis=1).astype(I32)


def place(span, begin, end, pos_ref, coords_ref, elem_ref, row_ref, group_ref, acc):
    size = acc.shape[0]
    wide = group_ref.shape[0]

    @pl.loop(begin, end)
    def _(it):
        hots, spreads = [], []
        for r in range(span):
            row = it * span + r
            group, at = split_position(pos_ref[pl.ds(row, 1), :], size)
            at = stack(rows16(at.astype(I32)), size // 16)
            hots.append(jnp.where(row_ref[0:size, :] == at, jnp.array(1, BF16), jnp.array(0, BF16)))
            lanes = pl.ds(pl.multiple_of(row * LANES, LANES), LANES)
            hi, lo = split2(coords_ref[:, lanes])
            elem = elem_ref[pl.ds(row, 1), :].astype(F32)
            values = jnp.concatenate([hi, elem, lo, jnp.zeros((1, LANES), F32)], axis=0)
            values = stack(stack(values, 2).astype(BF16), wide // 16)
            group = stack(rows16(group.astype(I32)), wide // 16)
            spreads.append(jnp.where(group_ref[...] == group, values, jnp.array(0, BF16)))
        acc[...] += dot_nt(jnp.concatenate(hots, axis=1), jnp.concatenate(spreads, axis=1))


def interpolate(elems, load, store, tiles, chunk, stacked, lag_ref, elem_rows):
    per = chunk // LANES
    for at in range(0, tiles, per):
        x = jnp.concatenate([load(at + t) for t in range(per)], axis=1)
        weights = []
        for d in range(3):
            coord = jnp.broadcast_to(x[d : d + 1], (8, chunk))
            const = [jnp.concatenate([lag_ref[r]] * per, axis=1) for r in range(8)]
            w = const[0] * (coord - const[1])
            for r in range(2, 8):
                w = w * (coord - const[r])
            weights.append(w)
        elem = stack(rows16(x[3:4].astype(I32)), elems // 16)
        pick = jnp.concatenate([elem_rows] * per, axis=1) == elem
        parts = []
        for part in split2(weights[0]):
            pieces = []
            for parity in range(2):
                for m in range(4):
                    i = 2 * m + parity
                    row = stack(jnp.broadcast_to(part[i : i + 1], (16, chunk)).astype(BF16), elems // 16)
                    pieces.append(jnp.where(pick, row, jnp.array(0, BF16)))
            parts.append(jnp.concatenate(pieces, axis=0))
        a_hi, a_lo = parts
        both = dot(stacked[...], a_hi)
        summed = both[0:192] + both[192:384] + dot(stacked[0:192], a_lo)
        results = []
        for c in range(3):
            total = None
            for j in range(8):
                term = summed[64 * c + 8 * j : 64 * c + 8 * j + 8] * weights[1][j : j + 1]
                total = term if total is None else total + term
            results.append(jnp.sum(total * weights[2], axis=0, keepdims=True))
        result = jnp.concatenate(results, axis=0)
        for t in range(per):
            store(at + t, result[:, LANES * t : LANES * (t + 1)])


def advect_kernel(
    outer, inner, tiles_each, sorted_tiles, chunk,
    vel_ref, coords_ref, owner_ref, elem_ref, nb_ref, tri_ref, low_ref, lag_ref, order_ref, back_ref, sel_t_ref,
    out_ref,
    pos_ref, meta_ref, meta_smem, row_ref, group_ref, acc, sorted_ref, send_ref, table_ref, mirror_ref,
    stacked, arrived, replies, landed, answers, halves, vals, faces, below, above,
    at_ref, group_of_ref, inner_ref,
    meta_sem, table_out, table_in, go_out, go_in, back_out, back_in, face_out, face_in,
):
    peers = outer * inner
    hin = inner // 2
    half = peers // 2
    elems = vel_ref.shape[1]
    points = coords_ref.shape[1]
    size = acc.shape[0]
    my_x, my_y = lax.axis_index("gx"), lax.axis_index("gy")
    side, low_y = my_y // hin, lax.rem(my_y, hin)
    me = my_x * inner + my_y
    mine = my_x * hin + low_y
    barrier = pltpu.get_barrier_semaphore()

    def place_of(device):
        return (device // inner, lax.rem(device, inner))

    @pl.loop(1, peers)
    def _(s):
        pl.semaphore_signal(barrier, inc=1, device_id=place_of(lax.rem(me + s, peers)), device_id_type=MESH)

    def code_base(p):
        x, y = p // inner, p % inner
        w = lax.rem(y // hin + side, 2)
        return (w * half + x * hin + y % hin) * tiles_each

    positions(peers, tiles_each, code_base, owner_ref, tri_ref, low_ref, pos_ref, meta_ref)
    meta_copy = pltpu.make_async_copy(meta_ref, meta_smem, meta_sem)
    meta_copy.start()

    row_ref[...] = lax.broadcasted_iota(I32, row_ref.shape, 0).astype(I16)
    group_ref[...] = (lax.broadcasted_iota(I32, group_ref.shape, 0) // 8).astype(I16)
    acc[...] = jnp.zeros_like(acc)
    for c in range(3):
        cube = vel_ref[c]
        tall = jnp.concatenate([cube[:, LANES * m : LANES * (m + 1)] for m in range(4)], axis=0).T
        table_ref[64 * c : 64 * (c + 1)] = jnp.concatenate([tall[0:64], tall[64:128]], axis=1)


    def halve(w, table):
        hi, lo = split2(table[...])
        stacked[w] = jnp.concatenate([hi, lo], axis=0).astype(BF16)

    halve(0, table_ref)

    span = 32
    steps = points // LANES // span
    place(span, 0, steps // 4, pos_ref, coords_ref, elem_ref, row_ref, group_ref, acc)
    pl.semaphore_wait(barrier, peers - 1)
    table_copy = pltpu.make_async_remote_copy(
        src_ref=table_ref, dst_ref=mirror_ref, send_sem=table_out, recv_sem=table_in,
        device_id=(my_x, lax.rem(my_y + hin, inner)), device_id_type=MESH,
    )
    table_copy.start()
    place(span, steps // 4, steps, pos_ref, coords_ref, elem_ref, row_ref, group_ref, acc)

    per_group = size // LANES
    for j in range(per_group):
        turned = acc[LANES * j : LANES * (j + 1), :].T
        for g in range(GROUPS):
            sorted_ref[g * per_group + j] = turned[8 * g : 8 * g + 8]
    for t in range(GROUPS * per_group, sorted_tiles):
        sorted_ref[t] = jnp.zeros((8, LANES), F32)

    def partner(s):
        device = mine ^ s
        return device, (device // hin, lax.rem(device, hin) + side * hin)

    def block(w, device):
        return pl.ds((w * half + device) * tiles_each, tiles_each)

    def remote(src, dst, out_sem, in_sem, w, s):
        device, where = partner(s)
        return pltpu.make_async_remote_copy(
            src_ref=src.at[block(w, device)], dst_ref=dst.at[block(w, mine)],
            send_sem=out_sem.at[w, device], recv_sem=in_sem.at[w, mine],
            device_id=where, device_id_type=MESH,
        )

    def arrival(src, dst, out_sem, in_sem, w, s):
        device, where = partner(s)
        return pltpu.make_async_remote_copy(
            src_ref=src.at[block(w, device)], dst_ref=dst.at[block(w, device)],
            send_sem=out_sem.at[w, device], recv_sem=in_sem.at[w, device],
            device_id=where, device_id_type=MESH,
        )

    outgoing = functools.partial(remote, send_ref, arrived, go_out, go_in)
    incoming = functools.partial(arrival, send_ref, arrived, go_out, go_in)
    reply = functools.partial(remote, replies, landed, back_out, back_in)
    answer = functools.partial(arrival, replies, landed, back_out, back_in)

    meta_copy.wait()

    def pack(into, w, s):
        device = mine ^ s
        owner = device // hin * inner + lax.rem(device, hin) + lax.rem(side + w, 2) * hin
        first = bounded(meta_smem[0, owner], sorted_tiles - tiles_each)
        base = (w * half + device) * tiles_each
        for k in range(tiles_each):
            into[base + k] = sorted_ref[first + k, 0:4, :] + sorted_ref[first + k, 4:8, :]

    def order(w, s):
        return s if w == 0 else half - s

    for w in range(2):
        @pl.loop(1, half)
        def _(s):
            pack(send_ref, w, order(w, s))
            outgoing(w, order(w, s)).start()

        pack(arrived, w, 0)

    pos = jnp.concatenate([pos_ref[pl.ds(r, elems, stride=4), :] for r in range(4)], axis=1)
    group, at = split_position(pos, PICK_ROWS)
    at_high = jnp.floor(at * 0.5)
    digits = jnp.concatenate([group, at_high, at - 2.0 * at_high], axis=0).astype(BF16)
    digits = dot(digits, order_ref[...])
    group_of_ref[...] = digits[0:elems].astype(I32)
    at_ref[...] = (2.0 * digits[elems : 2 * elems] + digits[2 * elems :]).astype(I32)

    elem_rows = row_ref[0:elems, :]
    together = 4
    turns = half // together

    @pl.loop(0, 2 * turns)
    def _(it):
        w, turn = it // turns, lax.rem(it, turns)

        @pl.when(it == turns)
        def _():
            table_copy.wait_recv()
            halve(1, mirror_ref)

        sources = []
        for u in range(together):
            s = together * turn + u
            s = s + w * (half - 1 - 2 * s)
            sources.append(s)

            @pl.when(s > 0)
            def _():
                incoming(w, s).wait_recv()

        for s in sources:
            base = (w * half + (mine ^ s)) * tiles_each

            def store(t, value):
                replies[base + t, 0:3, :] = value

            interpolate(
                elems, lambda t: arrived[base + t], store, tiles_each, chunk, stacked.at[w], lag_ref, elem_rows
            )
        for s in sources:
            @pl.when(s > 0)
            def _():
                reply(w, s).start()

    for w in range(2):
        own = (w * half + mine) * tiles_each
        for t in range(tiles_each):
            landed[own + t] = replies[own + t]

    table_copy.wait_send()
    for w in range(2):
        @pl.loop(1, half)
        def _(s):
            answer(w, s).wait_recv()

    groups = answers.shape[1] // 4
    per_row = PICK_ROWS // LANES
    for g in range(groups):
        for j in range(per_row):
            answers[j, 4 * g : 4 * g + 4, :] = landed[
                bounded(meta_smem[0, LANES + g * per_row + j], landed.shape[0] - 1)
            ]
    for c in range(3):
        rows = [answers[j, pl.ds(c, groups, stride=4), :] for j in range(per_row)]
        hi, lo = split2(jnp.concatenate(rows, axis=1))
        halves[groups * c : groups * (c + 1)] = hi.astype(BF16)
        halves[groups * (c + 3) : groups * (c + 4)] = lo.astype(BF16)

    up, down = lax.rem(me + 1, peers), lax.rem(me + peers - 1, peers)
    face_elems = elems // FACE_CHUNKS

    def pick(first, count, begin, width, store):
        def flat(ref):
            return jnp.concatenate([ref[pl.ds(first + u, 1), begin : begin + width] for u in range(count)], axis=1)

        at, group = flat(at_ref), flat(group_of_ref)
        at = stack(rows16(at), PICK_ROWS // 16)
        rows = jnp.concatenate([row_ref[0:PICK_ROWS, :]] * (count * width // LANES), axis=1)
        picked = dot(halves[...], jnp.where(rows == at, jnp.array(1, BF16), jnp.array(0, BF16)))
        match = lax.broadcasted_iota(I32, (groups, count * width), 0) == group
        for c in range(3):
            both = picked[groups * c : groups * (c + 1)] + picked[groups * (c + 3) : groups * (c + 4)]
            value = jnp.sum(jnp.where(match, both, 0.0), axis=0, keepdims=True)
            for u in range(count):
                store(c, u, value[:, width * u : width * (u + 1)])

    def face_copy(q, k):
        device, land = ((up, below), (down, above))[k]
        return pltpu.make_async_remote_copy(
            src_ref=faces.at[q], dst_ref=land.at[q],
            send_sem=face_out.at[q, k], recv_sem=face_in.at[q, k],
            device_id=place_of(device), device_id_type=MESH,
        )

    @pl.when(me == 0)
    def _():
        below[...] = jnp.zeros_like(below)

    @pl.when(me == peers - 1)
    def _():
        above[...] = jnp.zeros_like(above)

    step = 4
    per_chunk = face_elems // step

    @pl.loop(0, elems // step)
    def _(it):
        q, part = it // per_chunk, lax.rem(it, per_chunk)

        def store(c, u, value):
            faces[q, c, pl.ds(part * step + u, 1), :] = value

        pick(it * step, step, 0, 384, store)

        @pl.when((part == per_chunk - 1) & (me < peers - 1))
        def _():
            face_copy(q, 0).start()

        @pl.when((part == per_chunk - 1) & (me > 0))
        def _():
            face_copy(q, 1).start()

    inside = inner_ref.shape[2]

    @pl.loop(0, elems // step)
    def _(it):
        def store(c, u, value):
            inner_ref[c, pl.ds(it * step + u, 1), :] = value

        pick(it * step, step, 384, inside, store)

    index = (nb_ref[...] - jnp.where(nb_ref[...] >= 0, (me - 1) * elems, 0)).astype(F32)
    index = jnp.concatenate([index, jnp.zeros((2, elems), F32)], axis=0)
    index = jnp.concatenate([index] * (LANES // elems), axis=1).T[0:elems]
    columns = lax.broadcasted_iota(I32, (elems, 3 * elems), 1).astype(F32)
    column = [jnp.broadcast_to(index[:, f : f + 1], (elems, 3 * elems)) for f in range(6)]
    picker = jnp.concatenate([jnp.where(columns == column[f], 1.0, 0.0) for f in range(6)], axis=0).astype(BF16)
    present = [jnp.where(index[:, f : f + 1] >= 0, 0.5, 0.0) for f in range(6)]

    for w in range(2):
        @pl.loop(1, half)
        def _(s):
            outgoing(w, s).wait_send()
            reply(w, s).wait_send()

    def whole(ref, c):
        return jnp.concatenate([ref[q, c] for q in range(FACE_CHUNKS)], axis=0)

    def halves_of(x):
        hi, lo = split2(x)
        return hi.astype(BF16), lo.astype(BF16)

    def across_of(picks, parts):
        hi, lo = halves_of(jnp.concatenate(parts, axis=1))
        return dot(picks, hi) + dot(picks, lo)

    def moved(across, c):
        return jnp.concatenate(
            [across[f * elems : (f + 1) * elems, 384 * c + 64 * (f ^ 1) : 384 * c + 64 * (f ^ 1) + 64] for f in range(6)],
            axis=1,
        )

    own = [whole(faces, c) for c in range(3)]
    present = jnp.concatenate([jnp.broadcast_to(p, (elems, 64)) for p in present], axis=1)
    middle = across_of(picker[:, elems : 2 * elems], own)
    base = [0.5 * moved(middle, c) - present * own[c] for c in range(3)]
    kept = jnp.concatenate([jnp.concatenate([own[c], inner_ref[c]], axis=1) for c in range(3)], axis=0)
    hi, lo = halves_of(kept)
    spread = dot(jnp.concatenate([hi, lo], axis=0), back_ref[...])
    vals[...] = spread[: 3 * elems] + spread[3 * elems :]

    for q in range(FACE_CHUNKS):
        @pl.when(me < peers - 1)
        def _():
            face_copy(q, 0).wait_send()
            face_copy(q, 1).wait_recv()

        @pl.when(me > 0)
        def _():
            face_copy(q, 1).wait_send()
            face_copy(q, 0).wait_recv()

    picks = jnp.concatenate([picker[:, :elems], picker[:, 2 * elems :]], axis=1)
    outside = [jnp.concatenate([whole(below, c), whole(above, c)], axis=0) for c in range(3)]
    outside = across_of(picks, outside)
    hi, lo = halves_of(jnp.concatenate([base[c] + 0.5 * moved(outside, c) for c in range(3)], axis=0))
    spread = dot(jnp.concatenate([hi, lo], axis=0), sel_t_ref[...])
    for c in range(3):
        rows = slice(c * elems, (c + 1) * elems)
        out_ref[c] = vals[rows] + (spread[rows] + spread[(c + 3) * elems : (c + 4) * elems])


def advect(velocity, coords, owner, elem, neighbours, outer, inner):
    peers = outer * inner
    half = peers // 2
    elems = velocity.shape[1]
    points = coords.shape[1]
    capacity = 2 * points // peers
    tiles_each = capacity // LANES
    used = round_up(points // LANES + peers, GROUPS)
    size = used // GROUPS * LANES
    sorted_tiles = used + tiles_each
    groups = round_up(used * LANES, PICK_ROWS * 8) // PICK_ROWS
    code_lanes = round_up(groups * PICK_ROWS // LANES, LANES)
    tri = np.concatenate([np.triu(np.ones((LANES, LANES))), np.ones((LANES, LANES))], axis=1)
    low = np.tril(np.ones((points // LANES, points // LANES)), -1)
    order, back, sel_t = node_split()
    face_block = (FACE_CHUNKS, 3, elems // FACE_CHUNKS, 384)
    vmem = pl.BlockSpec(memory_space=pltpu.VMEM)
    return pl.pallas_call(
        functools.partial(advect_kernel, outer, inner, tiles_each, sorted_tiles, min(capacity, 256)),
        in_specs=[vmem] * 11,
        out_specs=vmem,
        out_shape=jax.ShapeDtypeStruct((3, elems, 512), F32),
        scratch_shapes=[
            pltpu.VMEM((points // LANES, LANES), F32),
            pltpu.VMEM((1, LANES + code_lanes), I32),
            pltpu.SMEM((1, LANES + code_lanes), I32),
            pltpu.VMEM((max(size, PICK_ROWS), LANES), I16),
            pltpu.VMEM((GROUPS * 8, LANES), I16),
            pltpu.VMEM((size, GROUPS * 8), F32),
            pltpu.VMEM((sorted_tiles, 8, LANES), F32),
            pltpu.VMEM((peers * tiles_each, 4, LANES), F32),
            pltpu.VMEM((192, elems * 8), F32),
            pltpu.VMEM((192, elems * 8), F32),
            pltpu.VMEM((2, 384, elems * 8), BF16),
            pltpu.VMEM((peers * tiles_each, 4, LANES), F32),
            pltpu.VMEM((peers * tiles_each, 4, LANES), F32),
            pltpu.VMEM((peers * tiles_each, 4, LANES), F32),
            pltpu.VMEM((PICK_ROWS // LANES, 4 * groups, LANES), F32),
            pltpu.VMEM((6 * groups, PICK_ROWS), BF16),
            pltpu.VMEM((3 * elems, 512), F32),
            pltpu.VMEM(face_block, F32),
            pltpu.VMEM(face_block, F32),
            pltpu.VMEM(face_block, F32),
            pltpu.VMEM((elems, order.shape[1]), I32),
            pltpu.VMEM((elems, order.shape[1]), I32),
            pltpu.VMEM((3, elems, order.shape[1] - 384), F32),
            pltpu.SemaphoreType.DMA,
            pltpu.SemaphoreType.DMA,
            pltpu.SemaphoreType.DMA,
        ]
        + [pltpu.SemaphoreType.DMA((2, half))] * 4
        + [pltpu.SemaphoreType.DMA((FACE_CHUNKS, 2))] * 2,
        compiler_params=pltpu.CompilerParams(collective_id=0, has_side_effects=True),
        name="advect",
    )(
        velocity, coords, owner, elem, neighbours, jnp.asarray(tri, BF16), jnp.asarray(low, BF16),
        jnp.asarray(lagrange_constants()),
        jnp.asarray(order, BF16), jnp.asarray(back, BF16), jnp.asarray(sel_t, BF16),
    )


def local(velocity, depart, owner_rank, owner_element_index, neighbours):
    outer, inner = lax.axis_size("gx"), lax.axis_size("gy")
    rows = depart.shape[1] // LANES
    owner = owner_rank.reshape(rows, LANES)
    elem = owner_element_index.reshape(rows, LANES)
    return advect(velocity, depart, owner, elem, neighbours, outer, inner)


def solution(mesh):
    placed = (
        P(None, ("gx", "gy"), None),
        P(None, ("gx", "gy")),
        P(("gx", "gy"), None),
        P(("gx", "gy")),
        P(None, ("gx", "gy")),
    )
    return jax.shard_map(
        local, mesh=mesh, in_specs=placed, out_specs=P(None, ("gx", "gy"), None), check_vma=False
    )
```

```python
import functools

import jax
import jax.numpy as jnp
import numpy as np
from jax import lax
from jax.experimental import pallas as pl
from jax.experimental.pallas import tpu as pltpu
from jax.sharding import PartitionSpec as P

GLL_POINTS = np.array(
    [
        -1.0,
        -0.8717401485096066,
        -0.5917001814331423,
        -0.2092992179024789,
        0.2092992179024789,
        0.5917001814331423,
        0.8717401485096066,
        1.0,
    ]
)
F32, BF16, I32, I16 = jnp.float32, jnp.bfloat16, jnp.int32, jnp.int16
MESH = pl.DeviceIdType.MESH
LANES = 128
GROUPS = 32
PICK_ROWS = 512
FACE_CHUNKS = 4


def lagrange_constants():
    table = np.zeros((8, 8, LANES))
    for i in range(8):
        table[0, i] = 1.0 / np.prod([GLL_POINTS[i] - GLL_POINTS[m] for m in range(8) if m != i])
        for r in range(1, 8):
            table[r, i] = GLL_POINTS[(i + r) % 8]
    return table.astype(np.float32)


def face_selector():
    cube = np.arange(512).reshape(8, 8, 8)
    faces = [cube[0], cube[7], cube[:, 0], cube[:, 7], cube[:, :, 0], cube[:, :, 7]]
    nodes = np.concatenate([face.reshape(-1) for face in faces])
    return (np.arange(512)[:, None] == nodes[None, :]).astype(np.float32)


def node_split():
    sel = face_selector()
    first = sel * (np.cumsum(sel, axis=1) == 1)
    inside = np.flatnonzero(sel.sum(axis=1) == 0)
    rest = np.zeros((512, round_up(len(inside), LANES)), np.float32)
    rest[inside, np.arange(len(inside))] = 1
    order = np.concatenate([sel, rest], axis=1)
    back = np.concatenate([first, rest, sel], axis=1).T
    return order, back


def round_up(x, to):
    return -(-x // to) * to


def split2(x):
    hi = x.astype(BF16).astype(F32)
    return hi, x - hi


def dot(a, b):
    return lax.dot_general(a, b, (((1,), (0,)), ((), ())), preferred_element_type=F32)


def dot_nt(a, b):
    return lax.dot_general(a, b, (((1,), (1,)), ((), ())), preferred_element_type=F32)


def rows16(row):
    return jnp.broadcast_to(row, (16, row.shape[1])).astype(I16)


def stack(tile, count):
    return jnp.concatenate([tile] * count, axis=0)


def bounded(index, most):
    return jnp.minimum(jnp.maximum(index, 0), most)


def split_position(pos, size):
    group = jnp.floor((pos + 0.5) * (1.0 / size))
    return group, pos - group * size


def positions(peers, tiles_each, code_base, owner_ref, tri_ref, low_ref, pos_ref, meta_ref):
    rows = owner_ref.shape[0]
    wide = meta_ref.shape[1] - LANES
    owner = owner_ref[...]
    lane = lax.broadcasted_iota(I32, (1, LANES), 1)
    tile_at = lax.broadcasted_iota(I32, (1, wide), 1).astype(F32)
    hots = [owner == p for p in range(peers)]
    ones = jnp.concatenate([jnp.where(hot, 1.0, 0.0).astype(BF16) for hot in hots], axis=1)
    ahead = dot(low_ref[...], ones)
    columns = [ahead[rows - 1 :, LANES * p : LANES * (p + 1)] for p in range(peers)]
    across = dot(jnp.concatenate(columns, axis=0).astype(BF16), tri_ref[...])
    tiles = jnp.floor((across[:, LANES:] + (LANES - 1.0)) * (1.0 / LANES))
    pos = jnp.zeros(owner.shape, F32)
    first = jnp.zeros((1, LANES), F32)
    starts, code = first, jnp.zeros((1, wide), F32)
    for p in range(peers):
        offset = across[p : p + 1, :LANES] + (first * LANES - 1.0)
        pos = jnp.where(hots[p], ahead[:, LANES * p : LANES * (p + 1)] + offset, pos)
        starts = jnp.where(lane == p, first, starts)
        begin = jnp.concatenate([first] * (wide // LANES), axis=1)
        here = code_base(p).astype(F32) + jnp.minimum(tile_at - begin, tiles_each - 1.0)
        code = jnp.where(tile_at >= begin, here, code)
        first = first + tiles[p : p + 1]
    pos_ref[...] = pos
    meta_ref[...] = jnp.concatenate([starts, code], axis=1).astype(I32)


def place(span, steps, ahead, pos_ref, coords_ref, elem_ref, row_ref, group_ref, acc):
    size = acc.shape[0]
    wide = group_ref.shape[0]

    @pl.loop(0, steps)
    def _(it):
        ahead(it)
        hots, spreads = [], []
        for r in range(span):
            row = it * span + r
            group, at = split_position(pos_ref[pl.ds(row, 1), :], size)
            at = stack(rows16(at.astype(I32)), size // 16)
            hots.append(jnp.where(row_ref[0:size, :] == at, jnp.array(1, BF16), jnp.array(0, BF16)))
            lanes = pl.ds(pl.multiple_of(row * LANES, LANES), LANES)
            hi, lo = split2(coords_ref[:, lanes])
            elem = elem_ref[pl.ds(row, 1), :].astype(F32)
            values = jnp.concatenate([hi, elem, lo, jnp.zeros((1, LANES), F32)], axis=0)
            values = stack(stack(values, 2).astype(BF16), wide // 16)
            group = stack(rows16(group.astype(I32)), wide // 16)
            spreads.append(jnp.where(group_ref[...] == group, values, jnp.array(0, BF16)))
        acc[...] += dot_nt(jnp.concatenate(hots, axis=1), jnp.concatenate(spreads, axis=1))


def interpolate(elems, load, store, tiles, chunk, stacked, lag_ref, elem_rows):
    per = chunk // LANES
    for at in range(0, tiles, per):
        x = jnp.concatenate([load(at + t) for t in range(per)], axis=1)
        weights = []
        for d in range(3):
            coord = jnp.broadcast_to(x[d : d + 1], (8, chunk))
            const = [jnp.concatenate([lag_ref[r]] * per, axis=1) for r in range(8)]
            w = const[0] * (coord - const[1])
            for r in range(2, 8):
                w = w * (coord - const[r])
            weights.append(w)
        elem = stack(rows16(x[3:4].astype(I32)), elems // 16)
        pick = jnp.concatenate([elem_rows] * per, axis=1) == elem
        parts = []
        for part in split2(weights[0]):
            pieces = []
            for parity in range(2):
                for m in range(4):
                    i = 2 * m + parity
                    row = stack(jnp.broadcast_to(part[i : i + 1], (16, chunk)).astype(BF16), elems // 16)
                    pieces.append(jnp.where(pick, row, jnp.array(0, BF16)))
            parts.append(jnp.concatenate(pieces, axis=0))
        a_hi, a_lo = parts
        both = dot(stacked[...], a_hi)
        summed = both[0:192] + both[192:384] + dot(stacked[0:192], a_lo)
        results = []
        for c in range(3):
            total = None
            for j in range(8):
                term = summed[64 * c + 8 * j : 64 * c + 8 * j + 8] * weights[1][j : j + 1]
                total = term if total is None else total + term
            results.append(jnp.sum(total * weights[2], axis=0, keepdims=True))
        result = jnp.concatenate(results, axis=0)
        for t in range(per):
            store(at + t, result[:, LANES * t : LANES * (t + 1)])


def advect_kernel(
    outer, inner, tiles_each, sorted_tiles, chunk,
    owner_hbm, tri_hbm, low_hbm, vel_hbm, coords_hbm, elem_hbm, nb_hbm, lag_hbm, order_hbm, back_hbm,
    out_ref,
    owner_ref, tri_ref, low_ref, vel_ref, coords_ref, elem_ref, nb_ref, lag_ref, order_ref, back_ref,
    load_sems,
    pos_ref, meta_ref, meta_smem, row_ref, group_ref, acc, sorted_ref, send_ref, table_ref, mirror_ref,
    stacked, arrived, replies, landed, answers, halves, faces, below, above,
    at_ref, group_of_ref, inner_ref, picker_ref, present_ref,
    meta_sem, table_out, table_in, go_out, go_in, back_out, back_in, face_out, face_in,
):
    peers = outer * inner
    hin = inner // 2
    half = peers // 2
    elems = vel_hbm.shape[1]
    points = coords_hbm.shape[1]
    size = acc.shape[0]
    my_x, my_y = lax.axis_index("gx"), lax.axis_index("gy")
    side, low_y = my_y // hin, lax.rem(my_y, hin)
    me = my_x * inner + my_y
    mine = my_x * hin + low_y
    barrier = pltpu.get_barrier_semaphore()
    loads = [
        pltpu.make_async_copy(src, dst, load_sems.at[i])
        for i, (src, dst) in enumerate((
            (owner_hbm, owner_ref), (tri_hbm, tri_ref), (low_hbm, low_ref), (vel_hbm, vel_ref), (coords_hbm, coords_ref),
            (elem_hbm, elem_ref), (nb_hbm, nb_ref), (lag_hbm, lag_ref), (order_hbm, order_ref), (back_hbm, back_ref),
        ))
    ]
    for copy in loads:
        copy.start()

    def load(stage, count):
        for copy in loads[stage : stage + count]:
            copy.wait()

    def place_of(device):
        return (device // inner, lax.rem(device, inner))

    @pl.loop(1, peers)
    def _(s):
        pl.semaphore_signal(barrier, inc=1, device_id=place_of(lax.rem(me + s, peers)), device_id_type=MESH)

    quarter = hin // 2

    def mirror(y):
        return (3 - y // quarter) * quarter + y % quarter

    def code_base(p):
        x, y = p // inner, p % inner
        w = lax.rem(y // hin + side, 2)
        low = y % hin + w * (mirror(y) % hin - y % hin)
        return (w * half + x * hin + low) * tiles_each

    load(0, 3)
    positions(peers, tiles_each, code_base, owner_ref, tri_ref, low_ref, pos_ref, meta_ref)
    meta_copy = pltpu.make_async_copy(meta_ref, meta_smem, meta_sem)
    meta_copy.start()

    row_ref[...] = lax.broadcasted_iota(I32, row_ref.shape, 0).astype(I16)
    group_ref[...] = (lax.broadcasted_iota(I32, group_ref.shape, 0) // 8).astype(I16)
    acc[...] = jnp.zeros_like(acc)
    load(3, 1)
    for c in range(3):
        cube = vel_ref[c]
        tall = jnp.concatenate([cube[:, LANES * m : LANES * (m + 1)] for m in range(4)], axis=0).T
        table_ref[64 * c : 64 * (c + 1)] = jnp.concatenate([tall[0:64], tall[64:128]], axis=1)


    def halve(w, table):
        hi, lo = split2(table[...])
        stacked[w] = jnp.concatenate([hi, lo], axis=0).astype(BF16)

    halve(0, table_ref)
    table_copy = pltpu.make_async_remote_copy(
        src_ref=table_ref, dst_ref=mirror_ref, send_sem=table_out, recv_sem=table_in,
        device_id=(my_x, (3 - my_y // quarter) * quarter + lax.rem(my_y, quarter)), device_id_type=MESH,
    )
    edge = my_y // quarter
    outer_edge = (edge == 0) | (edge == 3)

    load(4, 2)
    span = 32
    steps = points // LANES // span

    def ahead(it):
        @pl.when(it == 1)
        def _():
            pl.semaphore_wait(barrier, peers - 1)

        @pl.when((it == 1) & outer_edge)
        def _():
            table_copy.start()

        @pl.when((it == steps - 1) & jnp.logical_not(outer_edge))
        def _():
            table_copy.start()

    place(span, steps, ahead, pos_ref, coords_ref, elem_ref, row_ref, group_ref, acc)

    per_group = size // LANES
    for j in range(per_group):
        turned = acc[LANES * j : LANES * (j + 1), :].T
        for g in range(GROUPS):
            sorted_ref[g * per_group + j] = turned[8 * g : 8 * g + 8]
    for t in range(GROUPS * per_group, sorted_tiles):
        sorted_ref[t] = jnp.zeros((8, LANES), F32)

    def partner(s):
        device = mine ^ s
        return device, (device // hin, lax.rem(device, hin) + side * hin)

    def block(w, device):
        return pl.ds((w * half + device) * tiles_each, tiles_each)

    def remote(src, dst, out_sem, in_sem, w, s):
        device, where = partner(s)
        return pltpu.make_async_remote_copy(
            src_ref=src.at[block(w, device)], dst_ref=dst.at[block(w, mine)],
            send_sem=out_sem.at[w, device], recv_sem=in_sem.at[w, mine],
            device_id=where, device_id_type=MESH,
        )

    def arrival(src, dst, out_sem, in_sem, w, s):
        device, where = partner(s)
        return pltpu.make_async_remote_copy(
            src_ref=src.at[block(w, device)], dst_ref=dst.at[block(w, device)],
            send_sem=out_sem.at[w, device], recv_sem=in_sem.at[w, device],
            device_id=where, device_id_type=MESH,
        )

    outgoing = functools.partial(remote, send_ref, arrived, go_out, go_in)
    incoming = functools.partial(arrival, send_ref, arrived, go_out, go_in)
    reply = functools.partial(remote, replies, landed, back_out, back_in)
    answer = functools.partial(arrival, replies, landed, back_out, back_in)

    meta_copy.wait()

    def pack(into, w, s):
        device = mine ^ s
        y = lax.rem(device, hin) + side * hin
        if w == 1:
            y = (3 - y // quarter) * quarter + lax.rem(y, quarter)
        owner = device // hin * inner + y
        first = bounded(meta_smem[0, owner], sorted_tiles - tiles_each)
        base = (w * half + device) * tiles_each
        for k in range(tiles_each):
            into[base + k] = sorted_ref[first + k, 0:4, :] + sorted_ref[first + k, 4:8, :]

    def order(w, s):
        return s if w == 0 else half - s

    for w in range(2):
        batch = 3

        @pl.loop(0, (half - 1) // batch)
        def _(it):
            some = [order(w, 1 + it * batch + u) for u in range(batch)]
            for s in some:
                pack(send_ref, w, s)
            for s in some:
                outgoing(w, s).start()

        for s in range(1 + (half - 1) // batch * batch, half):
            pack(send_ref, w, order(w, s))
            outgoing(w, order(w, s)).start()

        pack(arrived, w, 0)

    load(6, 4)
    pos = jnp.concatenate([pos_ref[pl.ds(r, elems, stride=4), :] for r in range(4)], axis=1)
    group, at = split_position(pos, PICK_ROWS)
    at_high = jnp.floor(at * 0.5)
    digits = jnp.concatenate([group, at_high, at - 2.0 * at_high], axis=0).astype(BF16)
    digits = dot(digits, order_ref[...])
    group_of_ref[...] = digits[0:elems].astype(I32)
    at_ref[...] = (2.0 * digits[elems : 2 * elems] + digits[2 * elems :]).astype(I32)

    index = (nb_ref[...] - jnp.where(nb_ref[...] >= 0, (me - 1) * elems, 0)).astype(F32)
    index = jnp.concatenate([index, jnp.zeros((2, elems), F32)], axis=0)
    index = jnp.concatenate([index] * (LANES // elems), axis=1).T[0:elems]
    columns = lax.broadcasted_iota(I32, (elems, 3 * elems), 1).astype(F32)
    column = [jnp.broadcast_to(index[:, f : f + 1], (elems, 3 * elems)) for f in range(6)]
    picker = jnp.concatenate([jnp.where(columns == column[f], 1.0, 0.0) for f in range(6)], axis=0).astype(BF16)
    picker_ref[...] = picker
    present = [jnp.where(index[:, f : f + 1] >= 0, 0.5, 0.0) for f in range(6)]
    present_ref[...] = jnp.concatenate([jnp.broadcast_to(p, (elems, 64)) for p in present], axis=1)

    elem_rows = row_ref[0:elems, :]
    together = 4
    middle = half - 2

    def serve(sources):
        for w, s in sources:
            if not isinstance(s, int) or s > 0:
                incoming(w, s).wait_recv()
        for w, s in sources:
            base = (w * half + (mine ^ s)) * tiles_each

            def store(t, value):
                replies[base + t, 0:3, :] = value

            interpolate(
                elems, lambda t: arrived[base + t], store, tiles_each, chunk, stacked.at[w], lag_ref, elem_rows
            )
        for w, s in sources:
            if not isinstance(s, int) or s > 0:
                reply(w, s).start()

    serve([(0, 0), (0, 1)])

    @pl.loop(0, 2 * middle // together)
    def _(it):
        @pl.when(it == middle // together)
        def _():
            table_copy.wait_recv()
            halve(1, mirror_ref)

        sources = []
        for u in range(together):
            i = it * together + u
            w = i // middle
            sources.append((w, 2 + i + w * (2 * half - 5 - 2 * i)))
        serve(sources)

    serve([(1, 1), (1, 0)])

    for w in range(2):
        own = (w * half + mine) * tiles_each
        for t in range(tiles_each):
            landed[own + t] = replies[own + t]

    table_copy.wait_send()
    for w in range(2):
        @pl.loop(1, half)
        def _(s):
            answer(w, s).wait_recv()

    groups = answers.shape[1] // 4
    per_row = PICK_ROWS // LANES
    for g in range(groups):
        for j in range(per_row):
            answers[j, 4 * g : 4 * g + 4, :] = landed[
                bounded(meta_smem[0, LANES + g * per_row + j], landed.shape[0] - 1)
            ]
    for c in range(3):
        rows = [answers[j, pl.ds(c, groups, stride=4), :] for j in range(per_row)]
        hi, lo = split2(jnp.concatenate(rows, axis=1))
        halves[groups * c : groups * (c + 1)] = hi.astype(BF16)
        halves[groups * (c + 3) : groups * (c + 4)] = lo.astype(BF16)

    up, down = lax.rem(me + 1, peers), lax.rem(me + peers - 1, peers)
    face_elems = elems // FACE_CHUNKS

    def pick(first, count, begin, width, store):
        def flat(ref):
            return jnp.concatenate([ref[pl.ds(first + u, 1), begin : begin + width] for u in range(count)], axis=1)

        at, group = flat(at_ref), flat(group_of_ref)
        at = stack(rows16(at), PICK_ROWS // 16)
        rows = jnp.concatenate([row_ref[0:PICK_ROWS, :]] * (count * width // LANES), axis=1)
        picked = dot(halves[...], jnp.where(rows == at, jnp.array(1, BF16), jnp.array(0, BF16)))
        match = lax.broadcasted_iota(I32, (groups, count * width), 0) == group
        for c in range(3):
            both = picked[groups * c : groups * (c + 1)] + picked[groups * (c + 3) : groups * (c + 4)]
            value = jnp.sum(jnp.where(match, both, 0.0), axis=0, keepdims=True)
            for u in range(count):
                store(c, u, value[:, width * u : width * (u + 1)])

    def face_copy(q, k):
        device, land = ((up, below), (down, above))[k]
        return pltpu.make_async_remote_copy(
            src_ref=faces.at[q], dst_ref=land.at[q],
            send_sem=face_out.at[q, k], recv_sem=face_in.at[q, k],
            device_id=place_of(device), device_id_type=MESH,
        )

    @pl.when(me == 0)
    def _():
        below[...] = jnp.zeros_like(below)

    @pl.when(me == peers - 1)
    def _():
        above[...] = jnp.zeros_like(above)

    step = face_elems
    per_chunk = face_elems // step

    @pl.loop(0, elems // step)
    def _(it):
        q, part = it // per_chunk, lax.rem(it, per_chunk)

        def store(c, u, value):
            faces[q, c, pl.ds(part * step + u, 1), :] = value

        pick(it * step, step, 0, 384, store)

        @pl.when((part == per_chunk - 1) & (me < peers - 1))
        def _():
            face_copy(q, 0).start()

        @pl.when((part == per_chunk - 1) & (me > 0))
        def _():
            face_copy(q, 1).start()

    inside = inner_ref.shape[2]

    @pl.loop(0, elems // step)
    def _(it):
        def store(c, u, value):
            inner_ref[c, pl.ds(it * step + u, 1), :] = value

        pick(it * step, step, 384, inside, store)

    for w in range(2):
        @pl.loop(1, half)
        def _(s):
            outgoing(w, s).wait_send()
            reply(w, s).wait_send()

    def whole(ref, c):
        return jnp.concatenate([ref[q, c] for q in range(FACE_CHUNKS)], axis=0)

    def halves_of(x):
        hi, lo = split2(x)
        return hi.astype(BF16), lo.astype(BF16)

    def across_of(picks, parts):
        hi, lo = halves_of(jnp.concatenate(parts, axis=1))
        return dot(picks, hi) + dot(picks, lo)

    def moved(across, c):
        return jnp.concatenate(
            [across[f * elems : (f + 1) * elems, 384 * c + 64 * (f ^ 1) : 384 * c + 64 * (f ^ 1) + 64] for f in range(6)],
            axis=1,
        )

    for q in range(FACE_CHUNKS):
        @pl.when(me < peers - 1)
        def _():
            face_copy(q, 0).wait_send()
            face_copy(q, 1).wait_recv()

        @pl.when(me > 0)
        def _():
            face_copy(q, 1).wait_send()
            face_copy(q, 0).wait_recv()

    own = [whole(faces, c) for c in range(3)]
    extended = [jnp.concatenate([whole(below, c), own[c], whole(above, c)], axis=0) for c in range(3)]
    across = across_of(picker_ref[...], extended)
    present = present_ref[...]
    changes = [0.5 * moved(across, c) - present * own[c] for c in range(3)]
    hi, lo = halves_of(
        jnp.concatenate([jnp.concatenate([own[c], inner_ref[c], changes[c]], axis=1) for c in range(3)], axis=0)
    )
    spread = dot(jnp.concatenate([hi, lo], axis=0), back_ref[...])
    for c in range(3):
        out_ref[c] = spread[c * elems : (c + 1) * elems] + spread[(c + 3) * elems : (c + 4) * elems]


def advect(velocity, coords, owner, elem, neighbours, outer, inner):
    peers = outer * inner
    half = peers // 2
    elems = velocity.shape[1]
    points = coords.shape[1]
    capacity = 2 * points // peers
    tiles_each = capacity // LANES
    used = round_up(points // LANES + peers, GROUPS)
    size = used // GROUPS * LANES
    sorted_tiles = used + tiles_each
    groups = round_up(used * LANES, PICK_ROWS * 8) // PICK_ROWS
    code_lanes = round_up(groups * PICK_ROWS // LANES, LANES)
    tri = np.concatenate([np.triu(np.ones((LANES, LANES)), 1), np.ones((LANES, LANES))], axis=1)
    low = np.tril(np.ones((points // LANES, points // LANES)))
    order, back = node_split()
    face_block = (FACE_CHUNKS, 3, elems // FACE_CHUNKS, 384)
    vmem = pl.BlockSpec(memory_space=pltpu.VMEM)
    operands = (
        owner, jnp.asarray(tri, BF16), jnp.asarray(low, BF16), velocity, coords, elem, neighbours,
        jnp.asarray(lagrange_constants()), jnp.asarray(order, BF16), jnp.asarray(back, BF16),
    )
    return pl.pallas_call(
        functools.partial(advect_kernel, outer, inner, tiles_each, sorted_tiles, min(capacity, 256)),
        in_specs=[pl.BlockSpec(memory_space=pltpu.HBM)] * len(operands),
        out_specs=vmem,
        out_shape=jax.ShapeDtypeStruct((3, elems, 512), F32),
        scratch_shapes=[pltpu.VMEM(x.shape, x.dtype) for x in operands]
        + [
            pltpu.SemaphoreType.DMA((len(operands),)),
            pltpu.VMEM((points // LANES, LANES), F32),
            pltpu.VMEM((1, LANES + code_lanes), I32),
            pltpu.SMEM((1, LANES + code_lanes), I32),
            pltpu.VMEM((max(size, PICK_ROWS), LANES), I16),
            pltpu.VMEM((GROUPS * 8, LANES), I16),
            pltpu.VMEM((size, GROUPS * 8), F32),
            pltpu.VMEM((sorted_tiles, 8, LANES), F32),
            pltpu.VMEM((peers * tiles_each, 4, LANES), F32),
            pltpu.VMEM((192, elems * 8), F32),
            pltpu.VMEM((192, elems * 8), F32),
            pltpu.VMEM((2, 384, elems * 8), BF16),
            pltpu.VMEM((peers * tiles_each, 4, LANES), F32),
            pltpu.VMEM((peers * tiles_each, 4, LANES), F32),
            pltpu.VMEM((peers * tiles_each, 4, LANES), F32),
            pltpu.VMEM((PICK_ROWS // LANES, 4 * groups, LANES), F32),
            pltpu.VMEM((6 * groups, PICK_ROWS), BF16),
            pltpu.VMEM(face_block, F32),
            pltpu.VMEM(face_block, F32),
            pltpu.VMEM(face_block, F32),
            pltpu.VMEM((elems, order.shape[1]), I32),
            pltpu.VMEM((elems, order.shape[1]), I32),
            pltpu.VMEM((3, elems, order.shape[1] - 384), F32),
            pltpu.VMEM((6 * elems, 3 * elems), BF16),
            pltpu.VMEM((elems, 384), F32),
            pltpu.SemaphoreType.DMA,
            pltpu.SemaphoreType.DMA,
            pltpu.SemaphoreType.DMA,
        ]
        + [pltpu.SemaphoreType.DMA((2, half))] * 4
        + [pltpu.SemaphoreType.DMA((FACE_CHUNKS, 2))] * 2,
        compiler_params=pltpu.CompilerParams(collective_id=0, has_side_effects=True),
        name="advect",
    )(*operands)


def local(velocity, depart, owner_rank, owner_element_index, neighbours):
    outer, inner = lax.axis_size("gx"), lax.axis_size("gy")
    rows = depart.shape[1] // LANES
    owner = owner_rank.reshape(rows, LANES)
    elem = owner_element_index.reshape(rows, LANES)
    return advect(velocity, depart, owner, elem, neighbours, outer, inner)


def solution(mesh):
    placed = (
        P(None, ("gx", "gy"), None),
        P(None, ("gx", "gy")),
        P(("gx", "gy"), None),
        P(("gx", "gy")),
        P(None, ("gx", "gy")),
    )
    return jax.shard_map(
        local, mesh=mesh, in_specs=placed, out_specs=P(None, ("gx", "gy"), None), check_vma=False
    )
```

```python
import functools

import jax
import jax.numpy as jnp
import numpy as np
from jax import lax
from jax.experimental import pallas as pl
from jax.experimental.pallas import tpu as pltpu
from jax.sharding import PartitionSpec as P

GLL_POINTS = np.array(
    [
        -1.0,
        -0.8717401485096066,
        -0.5917001814331423,
        -0.2092992179024789,
        0.2092992179024789,
        0.5917001814331423,
        0.8717401485096066,
        1.0,
    ]
)
F32, BF16, I32, I16 = jnp.float32, jnp.bfloat16, jnp.int32, jnp.int16
MESH = pl.DeviceIdType.MESH
LANES = 128
GROUPS = 32
PICK_ROWS = 512
FACE_CHUNKS = 4


def lagrange_constants():
    table = np.zeros((8, 8, LANES))
    for i in range(8):
        table[0, i] = 1.0 / np.prod([GLL_POINTS[i] - GLL_POINTS[m] for m in range(8) if m != i])
        for r in range(1, 8):
            table[r, i] = GLL_POINTS[(i + r) % 8]
    return table.astype(np.float32)


def face_selector():
    cube = np.arange(512).reshape(8, 8, 8)
    faces = [cube[0], cube[7], cube[:, 0], cube[:, 7], cube[:, :, 0], cube[:, :, 7]]
    nodes = np.concatenate([face.reshape(-1) for face in faces])
    return (np.arange(512)[:, None] == nodes[None, :]).astype(np.float32)


def node_split():
    sel = face_selector()
    first = sel * (np.cumsum(sel, axis=1) == 1)
    inside = np.flatnonzero(sel.sum(axis=1) == 0)
    rest = np.zeros((512, round_up(len(inside), LANES)), np.float32)
    rest[inside, np.arange(len(inside))] = 1
    order = np.concatenate([sel, rest], axis=1)
    back = np.concatenate([first, rest, sel], axis=1).T
    return order, back


def round_up(x, to):
    return -(-x // to) * to


def split2(x):
    hi = x.astype(BF16).astype(F32)
    return hi, x - hi


def dot(a, b):
    return lax.dot_general(a, b, (((1,), (0,)), ((), ())), preferred_element_type=F32)


def dot_nt(a, b):
    return lax.dot_general(a, b, (((1,), (1,)), ((), ())), preferred_element_type=F32)


def rows16(row):
    return jnp.broadcast_to(row, (16, row.shape[1])).astype(I16)


def stack(tile, count):
    return jnp.concatenate([tile] * count, axis=0)


def bounded(index, most):
    return jnp.minimum(jnp.maximum(index, 0), most)


def split_position(pos, size):
    group = jnp.floor((pos + 0.5) * (1.0 / size))
    return group, pos - group * size


def positions(peers, tiles_each, code_base, owner_ref, tri_ref, low_ref, pos_ref, meta_ref):
    rows = owner_ref.shape[0]
    wide = meta_ref.shape[1] - LANES
    owner = owner_ref[...]
    lane = lax.broadcasted_iota(I32, (1, LANES), 1)
    tile_at = lax.broadcasted_iota(I32, (1, wide), 1).astype(F32)
    hots = [owner == p for p in range(peers)]
    ones = jnp.concatenate([jnp.where(hot, 1.0, 0.0).astype(BF16) for hot in hots], axis=1)
    ahead = dot(low_ref[...], ones)
    columns = [ahead[rows - 1 :, LANES * p : LANES * (p + 1)] for p in range(peers)]
    across = dot(jnp.concatenate(columns, axis=0).astype(BF16), tri_ref[...])
    tiles = jnp.floor((across[:, LANES:] + (LANES - 1.0)) * (1.0 / LANES))
    pos = jnp.zeros(owner.shape, F32)
    first = jnp.zeros((1, LANES), F32)
    starts, code = first, jnp.zeros((1, wide), F32)
    for p in range(peers):
        offset = across[p : p + 1, :LANES] + (first * LANES - 1.0)
        pos = jnp.where(hots[p], ahead[:, LANES * p : LANES * (p + 1)] + offset, pos)
        starts = jnp.where(lane == p, first, starts)
        begin = jnp.concatenate([first] * (wide // LANES), axis=1)
        here = code_base(p).astype(F32) + jnp.minimum(tile_at - begin, tiles_each - 1.0)
        code = jnp.where(tile_at >= begin, here, code)
        first = first + tiles[p : p + 1]
    pos_ref[...] = pos
    meta_ref[...] = jnp.concatenate([starts, code], axis=1).astype(I32)


def place(span, steps, ahead, pos_ref, coords_ref, elem_ref, row_ref, group_ref, acc):
    size = acc.shape[0]
    wide = group_ref.shape[0]

    @pl.loop(0, steps)
    def _(it):
        ahead(it)
        hots, spreads = [], []
        for r in range(span):
            row = it * span + r
            group, at = split_position(pos_ref[pl.ds(row, 1), :], size)
            at = stack(rows16(at.astype(I32)), size // 16)
            hots.append(jnp.where(row_ref[0:size, :] == at, jnp.array(1, BF16), jnp.array(0, BF16)))
            lanes = pl.ds(pl.multiple_of(row * LANES, LANES), LANES)
            hi, lo = split2(coords_ref[:, lanes])
            elem = elem_ref[pl.ds(row, 1), :].astype(F32)
            values = jnp.concatenate([hi, elem, lo, jnp.zeros((1, LANES), F32)], axis=0)
            values = stack(stack(values, 2).astype(BF16), wide // 16)
            group = stack(rows16(group.astype(I32)), wide // 16)
            spreads.append(jnp.where(group_ref[...] == group, values, jnp.array(0, BF16)))
        acc[...] += dot_nt(jnp.concatenate(hots, axis=1), jnp.concatenate(spreads, axis=1))


def interpolate(elems, load, store, tiles, chunk, stacked, lag_ref, elem_rows):
    per = chunk // LANES
    for at in range(0, tiles, per):
        x = jnp.concatenate([load(at + t) for t in range(per)], axis=1)
        weights = []
        for d in range(3):
            coord = jnp.broadcast_to(x[d : d + 1], (8, chunk))
            const = [jnp.concatenate([lag_ref[r]] * per, axis=1) for r in range(8)]
            w = const[0] * (coord - const[1])
            for r in range(2, 8):
                w = w * (coord - const[r])
            weights.append(w)
        elem = stack(rows16(x[3:4].astype(I32)), elems // 16)
        pick = jnp.concatenate([elem_rows] * per, axis=1) == elem
        parts = []
        for part in split2(weights[0]):
            pieces = []
            for parity in range(2):
                for m in range(4):
                    i = 2 * m + parity
                    row = stack(jnp.broadcast_to(part[i : i + 1], (16, chunk)).astype(BF16), elems // 16)
                    pieces.append(jnp.where(pick, row, jnp.array(0, BF16)))
            parts.append(jnp.concatenate(pieces, axis=0))
        a_hi, a_lo = parts
        both = dot(stacked[...], a_hi)
        summed = both[0:192] + both[192:384] + dot(stacked[0:192], a_lo)
        results = []
        for c in range(3):
            total = None
            for j in range(8):
                term = summed[64 * c + 8 * j : 64 * c + 8 * j + 8] * weights[1][j : j + 1]
                total = term if total is None else total + term
            results.append(jnp.sum(total * weights[2], axis=0, keepdims=True))
        result = jnp.concatenate(results, axis=0)
        for t in range(per):
            store(at + t, result[:, LANES * t : LANES * (t + 1)])


def advect_kernel(
    outer, inner, tiles_each, sorted_tiles, chunk,
    owner_hbm, tri_hbm, low_hbm, vel_hbm, coords_hbm, elem_hbm, nb_hbm, lag_hbm, order_hbm, back_hbm,
    out_ref,
    owner_ref, tri_ref, low_ref, vel_ref, coords_ref, elem_ref, nb_ref, lag_ref, order_ref, back_ref,
    load_sems,
    pos_ref, meta_ref, meta_smem, row_ref, group_ref, acc, sorted_ref, send_ref, table_ref, mirror_ref,
    stacked, arrived, replies, landed, answers, halves, faces, below, above,
    at_ref, group_of_ref, inner_ref, picker_ref, present_ref,
    meta_sem, table_out, table_in, go_out, go_in, back_out, back_in, face_out, face_in,
):
    peers = outer * inner
    hin = inner // 2
    half = peers // 2
    elems = vel_hbm.shape[1]
    points = coords_hbm.shape[1]
    size = acc.shape[0]
    my_x, my_y = lax.axis_index("gx"), lax.axis_index("gy")
    side, low_y = my_y // hin, lax.rem(my_y, hin)
    me = my_x * inner + my_y
    mine = my_x * hin + low_y
    barrier = pltpu.get_barrier_semaphore()
    loads = [
        pltpu.make_async_copy(src, dst, load_sems.at[i])
        for i, (src, dst) in enumerate((
            (owner_hbm, owner_ref), (tri_hbm, tri_ref), (low_hbm, low_ref), (vel_hbm, vel_ref), (coords_hbm, coords_ref),
            (elem_hbm, elem_ref), (nb_hbm, nb_ref), (lag_hbm, lag_ref), (order_hbm, order_ref), (back_hbm, back_ref),
        ))
    ]
    for copy in loads:
        copy.start()

    def load(stage, count):
        for copy in loads[stage : stage + count]:
            copy.wait()

    def place_of(device):
        return (device // inner, lax.rem(device, inner))

    @pl.loop(1, peers)
    def _(s):
        pl.semaphore_signal(barrier, inc=1, device_id=place_of(lax.rem(me + s, peers)), device_id_type=MESH)

    quarter = hin // 2

    def mirror(y):
        return (3 - y // quarter) * quarter + y % quarter

    def code_base(p):
        x, y = p // inner, p % inner
        w = lax.rem(y // hin + side, 2)
        low = y % hin + w * (mirror(y) % hin - y % hin)
        return (w * half + x * hin + low) * tiles_each

    load(0, 3)
    positions(peers, tiles_each, code_base, owner_ref, tri_ref, low_ref, pos_ref, meta_ref)
    meta_copy = pltpu.make_async_copy(meta_ref, meta_smem, meta_sem)
    meta_copy.start()

    row_ref[...] = lax.broadcasted_iota(I32, row_ref.shape, 0).astype(I16)
    group_ref[...] = (lax.broadcasted_iota(I32, group_ref.shape, 0) // 8).astype(I16)
    acc[...] = jnp.zeros_like(acc)
    load(3, 1)
    for c in range(3):
        cube = vel_ref[c]
        tall = jnp.concatenate([cube[:, LANES * m : LANES * (m + 1)] for m in range(4)], axis=0).T
        table_ref[64 * c : 64 * (c + 1)] = jnp.concatenate([tall[0:64], tall[64:128]], axis=1)


    def halve(w, table):
        hi, lo = split2(table[...])
        stacked[w] = jnp.concatenate([hi, lo], axis=0).astype(BF16)

    halve(0, table_ref)
    table_copy = pltpu.make_async_remote_copy(
        src_ref=table_ref, dst_ref=mirror_ref, send_sem=table_out, recv_sem=table_in,
        device_id=(my_x, (3 - my_y // quarter) * quarter + lax.rem(my_y, quarter)), device_id_type=MESH,
    )
    edge = my_y // quarter
    outer_edge = (edge == 0) | (edge == 3)

    load(4, 2)
    span = 64
    steps = points // LANES // span

    def ahead(it):
        @pl.when(it == 1)
        def _():
            pl.semaphore_wait(barrier, peers - 1)

        @pl.when((it == 1) & outer_edge)
        def _():
            table_copy.start()

    place(span, steps, ahead, pos_ref, coords_ref, elem_ref, row_ref, group_ref, acc)

    @pl.when(jnp.logical_not(outer_edge))
    def _():
        table_copy.start()

    per_group = size // LANES
    for j in range(per_group):
        turned = acc[LANES * j : LANES * (j + 1), :].T
        for g in range(GROUPS):
            sorted_ref[g * per_group + j] = turned[8 * g : 8 * g + 8]
    for t in range(GROUPS * per_group, sorted_tiles):
        sorted_ref[t] = jnp.zeros((8, LANES), F32)

    def partner(s):
        device = mine ^ s
        return device, (device // hin, lax.rem(device, hin) + side * hin)

    def block(w, device):
        return pl.ds((w * half + device) * tiles_each, tiles_each)

    def remote(src, dst, out_sem, in_sem, w, s):
        device, where = partner(s)
        return pltpu.make_async_remote_copy(
            src_ref=src.at[block(w, device)], dst_ref=dst.at[block(w, mine)],
            send_sem=out_sem.at[w, device], recv_sem=in_sem.at[w, mine],
            device_id=where, device_id_type=MESH,
        )

    def arrival(src, dst, out_sem, in_sem, w, s):
        device, where = partner(s)
        return pltpu.make_async_remote_copy(
            src_ref=src.at[block(w, device)], dst_ref=dst.at[block(w, device)],
            send_sem=out_sem.at[w, device], recv_sem=in_sem.at[w, device],
            device_id=where, device_id_type=MESH,
        )

    outgoing = functools.partial(remote, send_ref, arrived, go_out, go_in)
    incoming = functools.partial(arrival, send_ref, arrived, go_out, go_in)
    reply = functools.partial(remote, replies, landed, back_out, back_in)
    answer = functools.partial(arrival, replies, landed, back_out, back_in)

    meta_copy.wait()

    def pack(into, w, s):
        device = mine ^ s
        y = lax.rem(device, hin) + side * hin
        if w == 1:
            y = (3 - y // quarter) * quarter + lax.rem(y, quarter)
        owner = device // hin * inner + y
        first = bounded(meta_smem[0, owner], sorted_tiles - tiles_each)
        base = (w * half + device) * tiles_each
        for k in range(tiles_each):
            into[base + k] = sorted_ref[first + k, 0:4, :] + sorted_ref[first + k, 4:8, :]

    def order(w, s):
        return s if w == 0 else half - s

    for w in range(2):
        batch = 3

        @pl.loop(0, (half - 1) // batch)
        def _(it):
            some = [order(w, 1 + it * batch + u) for u in range(batch)]
            for s in some:
                pack(send_ref, w, s)
            for s in some:
                outgoing(w, s).start()

        for s in range(1 + (half - 1) // batch * batch, half):
            pack(send_ref, w, order(w, s))
            outgoing(w, order(w, s)).start()

        pack(arrived, w, 0)

    load(6, 4)
    pos = jnp.concatenate([pos_ref[pl.ds(r, elems, stride=4), :] for r in range(4)], axis=1)
    group, at = split_position(pos, PICK_ROWS)
    at_high = jnp.floor(at * 0.5)
    digits = jnp.concatenate([group, at_high, at - 2.0 * at_high], axis=0).astype(BF16)
    digits = dot(digits, order_ref[...])
    group_of_ref[...] = digits[0:elems].astype(I32)
    at_ref[...] = (2.0 * digits[elems : 2 * elems] + digits[2 * elems :]).astype(I32)

    index = (nb_ref[...] - jnp.where(nb_ref[...] >= 0, (me - 1) * elems, 0)).astype(F32)
    index = jnp.concatenate([index, jnp.zeros((2, elems), F32)], axis=0)
    index = jnp.concatenate([index] * (LANES // elems), axis=1).T[0:elems]
    columns = lax.broadcasted_iota(I32, (elems, 3 * elems), 1).astype(F32)
    column = [jnp.broadcast_to(index[:, f : f + 1], (elems, 3 * elems)) for f in range(6)]
    picker = jnp.concatenate([jnp.where(columns == column[f], 1.0, 0.0) for f in range(6)], axis=0).astype(BF16)
    picker_ref[...] = picker
    present = [jnp.where(index[:, f : f + 1] >= 0, 0.5, 0.0) for f in range(6)]
    present_ref[...] = jnp.concatenate([jnp.broadcast_to(p, (elems, 64)) for p in present], axis=1)

    elem_rows = row_ref[0:elems, :]
    together = 7
    middle = half - 2

    def serve(sources):
        for w, s in sources:
            if not isinstance(s, int) or s > 0:
                incoming(w, s).wait_recv()
        for w, s in sources:
            base = (w * half + (mine ^ s)) * tiles_each

            def store(t, value):
                replies[base + t, 0:3, :] = value

            interpolate(
                elems, lambda t: arrived[base + t], store, tiles_each, chunk, stacked.at[w], lag_ref, elem_rows
            )
        for w, s in sources:
            if not isinstance(s, int) or s > 0:
                reply(w, s).start()

    serve([(0, 0), (0, 1)])

    @pl.loop(0, 2 * middle // together)
    def _(it):
        @pl.when(it == middle // together)
        def _():
            table_copy.wait_recv()
            halve(1, mirror_ref)

        sources = []
        for u in range(together):
            i = it * together + u
            w = i // middle
            sources.append((w, 2 + i + w * (2 * half - 5 - 2 * i)))
        serve(sources)

    serve([(1, 1), (1, 0)])

    for w in range(2):
        own = (w * half + mine) * tiles_each
        for t in range(tiles_each):
            landed[own + t] = replies[own + t]

    table_copy.wait_send()
    for w in range(2):
        @pl.loop(1, half)
        def _(s):
            answer(w, s).wait_recv()

    groups = answers.shape[1] // 4
    per_row = PICK_ROWS // LANES
    for g in range(groups):
        for j in range(per_row):
            answers[j, 4 * g : 4 * g + 4, :] = landed[
                bounded(meta_smem[0, LANES + g * per_row + j], landed.shape[0] - 1)
            ]
    for c in range(3):
        rows = [answers[j, pl.ds(c, groups, stride=4), :] for j in range(per_row)]
        hi, lo = split2(jnp.concatenate(rows, axis=1))
        halves[groups * c : groups * (c + 1)] = hi.astype(BF16)
        halves[groups * (c + 3) : groups * (c + 4)] = lo.astype(BF16)

    up, down = lax.rem(me + 1, peers), lax.rem(me + peers - 1, peers)
    face_elems = elems // FACE_CHUNKS

    def pick(first, count, begin, width, store):
        def flat(ref):
            return jnp.concatenate([ref[pl.ds(first + u, 1), begin : begin + width] for u in range(count)], axis=1)

        at, group = flat(at_ref), flat(group_of_ref)
        at = stack(rows16(at), PICK_ROWS // 16)
        rows = jnp.concatenate([row_ref[0:PICK_ROWS, :]] * (count * width // LANES), axis=1)
        picked = dot(halves[...], jnp.where(rows == at, jnp.array(1, BF16), jnp.array(0, BF16)))
        match = lax.broadcasted_iota(I32, (groups, count * width), 0) == group
        for c in range(3):
            both = picked[groups * c : groups * (c + 1)] + picked[groups * (c + 3) : groups * (c + 4)]
            value = jnp.sum(jnp.where(match, both, 0.0), axis=0, keepdims=True)
            for u in range(count):
                store(c, u, value[:, width * u : width * (u + 1)])

    def face_copy(q, k):
        device, land = ((up, below), (down, above))[k]
        return pltpu.make_async_remote_copy(
            src_ref=faces.at[q], dst_ref=land.at[q],
            send_sem=face_out.at[q, k], recv_sem=face_in.at[q, k],
            device_id=place_of(device), device_id_type=MESH,
        )

    @pl.when(me == 0)
    def _():
        below[...] = jnp.zeros_like(below)

    @pl.when(me == peers - 1)
    def _():
        above[...] = jnp.zeros_like(above)

    step = face_elems
    per_chunk = face_elems // step

    @pl.loop(0, elems // step)
    def _(it):
        q, part = it // per_chunk, lax.rem(it, per_chunk)

        def store(c, u, value):
            faces[q, c, pl.ds(part * step + u, 1), :] = value

        pick(it * step, step, 0, 384, store)

        @pl.when((part == per_chunk - 1) & (me < peers - 1))
        def _():
            face_copy(q, 0).start()

        @pl.when((part == per_chunk - 1) & (me > 0))
        def _():
            face_copy(q, 1).start()

    inside = inner_ref.shape[2]

    @pl.loop(0, elems // step)
    def _(it):
        def store(c, u, value):
            inner_ref[c, pl.ds(it * step + u, 1), :] = value

        pick(it * step, step, 384, inside, store)

    for w in range(2):
        @pl.loop(1, half)
        def _(s):
            outgoing(w, s).wait_send()
            reply(w, s).wait_send()

    def whole(ref, c):
        return jnp.concatenate([ref[q, c] for q in range(FACE_CHUNKS)], axis=0)

    def halves_of(x):
        hi, lo = split2(x)
        return hi.astype(BF16), lo.astype(BF16)

    def across_of(picks, parts):
        hi, lo = halves_of(jnp.concatenate(parts, axis=1))
        return dot(picks, hi) + dot(picks, lo)

    def moved(across, c):
        return jnp.concatenate(
            [across[f * elems : (f + 1) * elems, 384 * c + 64 * (f ^ 1) : 384 * c + 64 * (f ^ 1) + 64] for f in range(6)],
            axis=1,
        )

    for q in range(FACE_CHUNKS):
        @pl.when(me < peers - 1)
        def _():
            face_copy(q, 0).wait_send()
            face_copy(q, 1).wait_recv()

        @pl.when(me > 0)
        def _():
            face_copy(q, 1).wait_send()
            face_copy(q, 0).wait_recv()

    own = [whole(faces, c) for c in range(3)]
    extended = [jnp.concatenate([whole(below, c), own[c], whole(above, c)], axis=0) for c in range(3)]
    across = across_of(picker_ref[...], extended)
    present = present_ref[...]
    changes = [0.5 * moved(across, c) - present * own[c] for c in range(3)]
    hi, lo = halves_of(
        jnp.concatenate([jnp.concatenate([own[c], inner_ref[c], changes[c]], axis=1) for c in range(3)], axis=0)
    )
    spread = dot(jnp.concatenate([hi, lo], axis=0), back_ref[...])
    for c in range(3):
        out_ref[c] = spread[c * elems : (c + 1) * elems] + spread[(c + 3) * elems : (c + 4) * elems]


def advect(velocity, coords, owner, elem, neighbours, outer, inner):
    peers = outer * inner
    half = peers // 2
    elems = velocity.shape[1]
    points = coords.shape[1]
    capacity = 2 * points // peers
    tiles_each = capacity // LANES
    used = round_up(points // LANES + peers, GROUPS)
    size = used // GROUPS * LANES
    sorted_tiles = used + tiles_each
    groups = round_up(used * LANES, PICK_ROWS * 8) // PICK_ROWS
    code_lanes = round_up(groups * PICK_ROWS // LANES, LANES)
    tri = np.concatenate([np.triu(np.ones((LANES, LANES)), 1), np.ones((LANES, LANES))], axis=1)
    low = np.tril(np.ones((points // LANES, points // LANES)))
    order, back = node_split()
    face_block = (FACE_CHUNKS, 3, elems // FACE_CHUNKS, 384)
    vmem = pl.BlockSpec(memory_space=pltpu.VMEM)
    operands = (
        owner, jnp.asarray(tri, BF16), jnp.asarray(low, BF16), velocity, coords, elem, neighbours,
        jnp.asarray(lagrange_constants()), jnp.asarray(order, BF16), jnp.asarray(back, BF16),
    )
    return pl.pallas_call(
        functools.partial(advect_kernel, outer, inner, tiles_each, sorted_tiles, min(capacity, 256)),
        in_specs=[pl.BlockSpec(memory_space=pltpu.HBM)] * len(operands),
        out_specs=vmem,
        out_shape=jax.ShapeDtypeStruct((3, elems, 512), F32),
        scratch_shapes=[pltpu.VMEM(x.shape, x.dtype) for x in operands]
        + [
            pltpu.SemaphoreType.DMA((len(operands),)),
            pltpu.VMEM((points // LANES, LANES), F32),
            pltpu.VMEM((1, LANES + code_lanes), I32),
            pltpu.SMEM((1, LANES + code_lanes), I32),
            pltpu.VMEM((max(size, PICK_ROWS), LANES), I16),
            pltpu.VMEM((GROUPS * 8, LANES), I16),
            pltpu.VMEM((size, GROUPS * 8), F32),
            pltpu.VMEM((sorted_tiles, 8, LANES), F32),
            pltpu.VMEM((peers * tiles_each, 4, LANES), F32),
            pltpu.VMEM((192, elems * 8), F32),
            pltpu.VMEM((192, elems * 8), F32),
            pltpu.VMEM((2, 384, elems * 8), BF16),
            pltpu.VMEM((peers * tiles_each, 4, LANES), F32),
            pltpu.VMEM((peers * tiles_each, 4, LANES), F32),
            pltpu.VMEM((peers * tiles_each, 4, LANES), F32),
            pltpu.VMEM((PICK_ROWS // LANES, 4 * groups, LANES), F32),
            pltpu.VMEM((6 * groups, PICK_ROWS), BF16),
            pltpu.VMEM(face_block, F32),
            pltpu.VMEM(face_block, F32),
            pltpu.VMEM(face_block, F32),
            pltpu.VMEM((elems, order.shape[1]), I32),
            pltpu.VMEM((elems, order.shape[1]), I32),
            pltpu.VMEM((3, elems, order.shape[1] - 384), F32),
            pltpu.VMEM((6 * elems, 3 * elems), BF16),
            pltpu.VMEM((elems, 384), F32),
            pltpu.SemaphoreType.DMA,
            pltpu.SemaphoreType.DMA,
            pltpu.SemaphoreType.DMA,
        ]
        + [pltpu.SemaphoreType.DMA((2, half))] * 4
        + [pltpu.SemaphoreType.DMA((FACE_CHUNKS, 2))] * 2,
        compiler_params=pltpu.CompilerParams(collective_id=0, has_side_effects=True),
        name="advect",
    )(*operands)


def local(velocity, depart, owner_rank, owner_element_index, neighbours):
    outer, inner = lax.axis_size("gx"), lax.axis_size("gy")
    rows = depart.shape[1] // LANES
    owner = owner_rank.reshape(rows, LANES)
    elem = owner_element_index.reshape(rows, LANES)
    return advect(velocity, depart, owner, elem, neighbours, outer, inner)


def solution(mesh):
    placed = (
        P(None, ("gx", "gy"), None),
        P(None, ("gx", "gy")),
        P(("gx", "gy"), None),
        P(("gx", "gy")),
        P(None, ("gx", "gy")),
    )
    return jax.shard_map(
        local, mesh=mesh, in_specs=placed, out_specs=P(None, ("gx", "gy"), None), check_vma=False
    )
```
